32 devices in a mesh: det: 4 (over y, core), tm: 8 (over z, x).
Axes of the slice: x: 2, y: 2, z: 4, core: 2. Of those that a mesh axis runs over, the one named last changes fastest.
Arguments:
- spectra: bfloat16 [4, 16, 32, 2, 128], P('det', 'tm'), may hold values from -200 to 200
- valid: int32 [16], P('tm'), may hold values 0 or 1
- lags: float32 [49152], replicated, may hold values from -0.01 to 0.01
- drift: float32 [49152], replicated, may hold values from -4 to 4
- block_table: int32 [64, 2], replicated, may hold values from 0 to 95, as said below
Outputs:
- sky_map: float32 [49152], P(('det', 'tm'))
The draws below stay inside these ranges and needn't reach their ends.
Inputs may be any that keep to these rules, and one draw needn't show every extreme that they name: `block_table`: row (2 i + h) * 4 + k, for 0 <= i < 8, h in 0, 1 and 0 <= k < 4, holds a band from h * 32 to h * 32 + 31 and a tile below 96; each aligned block of 2 rows starting at a multiple of 2 has one band, and the 2 bands of one (i, h) are distinct.
All inputs are finite; a program needn't handle non-finite values. No bound on the sum of `valid` on one device may be relied on, other than what follows from the above.
Results may differ from the reference program's by a relative error of at most 0.0037.
Values may be sent and summed in bfloat16 or wider, within the bound.
No kernel may reach another device: no remote copies, remote signals or barrier semaphores. Data moves between devices by JAX's collectives and lax.ppermute only.
A program may use at most 64 MiB of HBM per device.

```python
import math
import jax
import jax.numpy as jnp
from jax import lax

F = 8192
P_SIZE = 49152
BW = 128
PT = 512
TPB = 2
BLK_DEV = 4
NBH = 32
NBAND = 64
NTILE = 96
SEGS = 16
NBLK = 64
BAND_DEV = 2
N_TM = 8


def draw_spectra(key, part):
    noise_key = jax.random.fold_in(key, 0)
    shape = (4, SEGS, NBH, 2, BW)
    bin_half = jnp.arange(4, dtype=jnp.int32) % 2
    position = (bin_half[:, None, None] * (NBH * BW) + jnp.arange(NBH, dtype=jnp.int32)[None, :, None] * BW + jnp.arange(BW, dtype=jnp.int32)[None, None, :]).astype(jnp.float32) / F
    envelope = jnp.power(3.0, 1.0 - position)
    noise_values = jax.random.normal(noise_key, shape, jnp.float32)
    result = noise_values * envelope[:, None, :, None, :]
    return result.astype(jnp.bfloat16)


def pick_bands(band_key):
    return jax.random.permutation(band_key, NBH)[:BAND_DEV]


def draw_block_table(key, part):
    band_key, tile_key = jax.random.split(jax.random.fold_in(key, 7))
    groups = N_TM * 2
    picked = jax.vmap(pick_bands)(jax.random.split(band_key, groups)).astype(jnp.int32)
    offsets = jnp.arange(groups, dtype=jnp.int32) % 2 * NBH
    bands = jnp.repeat(picked + offsets[:, None], TPB, axis=1)
    tile_ids = jax.random.randint(tile_key, (groups, BLK_DEV), 0, NTILE, dtype=jnp.int32)
    return jnp.stack([bands, tile_ids], -1).reshape(NBLK, 2).astype(jnp.int32)


def plant(drawn, key, least, high):
    extent = drawn.shape
    index_at = [jax.random.randint(jax.random.fold_in(key, axis), (), 0, extent[axis]) for axis in range(len(extent))]
    drawn = drawn.at[tuple(index_at)].set(least)
    longest = extent.index(max(extent))
    index_at[longest] = (index_at[longest] + 1) % extent[longest]
    return drawn.at[tuple(index_at)].set(high)


def setup_inputs(seed: int = 0) -> dict:
    key_of = jax.random.split(jax.random.key(seed), 6)
    spectra = draw_spectra(jax.random.fold_in(key_of[5], 71), 0)
    valid = plant((jax.random.randint(key_of[1], (SEGS,), 0, 4) < 3).astype(jnp.int32), jax.random.fold_in(key_of[1], 1), 0, 1)
    lags = jnp.clip(jax.random.uniform(key_of[2], (P_SIZE,), jnp.float32, -0.01, 0.01), -0.01, 0.01)
    drift = jnp.clip(jax.random.uniform(key_of[3], (P_SIZE,), jnp.float32, -4.0, 4.0), -4.0, 4.0)
    block_table = draw_block_table(jax.random.fold_in(key_of[5], 71), 0)
    return {"spectra": spectra, "valid": valid, "lags": lags, "drift": drift, "block_table": block_table}


full_turn = 2.0 * math.pi

def tile_partial(band_slab, band_id, pixel_lags, pixel_drift, time_coord, band_total, band_width):
    frequency = (band_id * band_width + jnp.arange(band_width, dtype=jnp.int32)).astype(jnp.float32)
    angle_grid = full_turn * frequency[:, None] * pixel_lags[None, :]
    cosine_grid = jnp.cos(angle_grid)
    sine_grid = jnp.sin(angle_grid)
    kernel = jnp.concatenate([jnp.concatenate([cosine_grid, -sine_grid], 1), jnp.concatenate([sine_grid, cosine_grid], 1)], 0).astype(jnp.bfloat16)
    product = jnp.dot(band_slab.astype(jnp.float32), kernel.astype(jnp.float32), precision=lax.Precision.HIGHEST, preferred_element_type=jnp.float32)
    columns = pixel_lags.shape[0]
    factor = full_turn * (band_id.astype(jnp.float32) + 0.5) / band_total
    rotation = (factor * pixel_drift)[None, :] * time_coord[:, None]
    return lax.optimization_barrier(jnp.sum(jnp.cos(rotation) * product[:, :columns] - jnp.sin(rotation) * product[:, columns:], axis=0))

def reference(spectra, valid, lags, drift, block_table):
    values = spectra.astype(jnp.float32)
    squares = lax.optimization_barrier(jnp.sum(values * values, axis=(2, 3, 4)))
    powers = squares.reshape(2, 2, SEGS).sum(axis=1) / F + 1e-06
    weight = valid.astype(jnp.float32) / (powers[0] * powers[1])
    hanford = jnp.concatenate([values[0], values[1]], axis=1)
    livingston = jnp.concatenate([values[2], values[3]], axis=1)
    cross_real = (hanford[:, :, 0] * livingston[:, :, 0] + hanford[:, :, 1] * livingston[:, :, 1]) * weight[:, None, None]
    cross_imag = (hanford[:, :, 0] * livingston[:, :, 1] - hanford[:, :, 1] * livingston[:, :, 0]) * weight[:, None, None]
    cross = jnp.stack([cross_real, cross_imag], 2).astype(jnp.bfloat16).reshape(SEGS, NBAND, 2 * BW)
    time_coord = (jnp.arange(SEGS, dtype=jnp.int32).astype(jnp.float32) + 0.5 - SEGS / 2) / SEGS

    def one_block(block_row):
        band_slab = lax.dynamic_index_in_dim(cross, block_row[0], 1, keepdims=False)
        pixel_start = block_row[1] * PT
        pixel_lags = lax.dynamic_slice_in_dim(lags, pixel_start, PT)
        pixel_drift = lax.dynamic_slice_in_dim(drift, pixel_start, PT)
        return tile_partial(band_slab, block_row[0], pixel_lags, pixel_drift, time_coord, NBAND, BW)
    partials = lax.map(one_block, block_table)
    summed = jax.ops.segment_sum(partials, block_table[:, 1], num_segments=NTILE)
    return summed.reshape(P_SIZE) / math.sqrt(SEGS * BW)
```

```python
import functools
import math

import jax
import jax.numpy as jnp
import numpy as np
from jax import lax
from jax.experimental import pallas as pl
from jax.experimental.pallas import tpu as pltpu
from jax.sharding import PartitionSpec as P

PT = 512
TPB = 2
LANES = 128
INNER = 16
PARTS = 6

NEAR_COS = (0.9999999994443334, -19.739207715972064, 64.93905415215964, -85.41956519425082, 58.57456432893444)
NEAR_SIN = (6.283185306861161, -41.341701618023556, 81.60505457483515, -76.68452620857785, 41.10289536853278)
VMEM = pl.BlockSpec(memory_space=pltpu.VMEM)
SMEM = pl.BlockSpec(memory_space=pltpu.SMEM)


def fitted(function, limit, degree):
    nodes = (np.cos(np.pi * (np.arange(400) + 0.5) / 400) + 1) / 2
    powers = np.vander(nodes, degree + 1, increasing=True)
    coefficients = np.linalg.lstsq(powers, function(np.sqrt(nodes * limit)), rcond=None)[0]
    return tuple(float(c) for c in coefficients / limit ** np.arange(degree + 1))


FAR_COS = fitted(lambda r: np.cos(2 * np.pi * r), 0.25, 6)
FAR_SIN = fitted(lambda r: np.sin(2 * np.pi * r) / r, 0.25, 6)


def horner(coefficients, z):
    total = jnp.full_like(z, coefficients[-1])
    for c in coefficients[-2::-1]:
        total = total * z + c
    return total


def near_turn(x):
    z = x * x
    return horner(NEAR_COS, z), x * horner(NEAR_SIN, z)


def any_turn(x):
    r = x - jnp.floor(x + 0.5)
    z = r * r
    return horner(FAR_COS, z), r * horner(FAR_SIN, z)


def split(x):
    high = x.astype(jnp.bfloat16)
    return high, (x - high.astype(jnp.float32)).astype(jnp.bfloat16)


def terms_kernel(
    tm_count, rows_dest, seg_kept,
    place_ref, valid_ref, table_ref, own_ref, other_ref, lags_ref, drift_ref,
    out_ref,
    own32, other32, cross, masked, left, total,
):
    det_index, tm_index = place_ref[0], place_ref[1]
    bin_half = det_index % 2
    detector_bit = det_index // 2
    bands_half = own_ref.shape[1] // 2
    width = own_ref.shape[2]
    outer = width // INNER
    seg_count = own_ref.shape[0]
    segment_total = seg_count * tm_count
    band_total = 2 * bands_half
    per_group = table_ref.shape[1] // (2 * tm_count)
    slots = tm_count * per_group // TPB
    per_tile = PT // LANES
    flip = jnp.where(detector_bit == 0, 1.0, -1.0).astype(jnp.float32)
    outer_at = lax.broadcasted_iota(jnp.int32, (outer, width), 0)
    lane_at = lax.broadcasted_iota(jnp.int32, (outer, width), 1)
    mask = (lane_at // INNER == outer_at).astype(jnp.float32)
    from_lane = lax.broadcasted_iota(jnp.int32, (width, LANES), 0) % INNER
    to_lane = lax.broadcasted_iota(jnp.int32, (width, LANES), 1)
    same = from_lane == to_lane % INNER
    part = to_lane // INNER

    def chooser(*parts):
        chosen = part == parts[0]
        for p in parts[1:]:
            chosen = chosen | (part == p)
        return (same & chosen).astype(jnp.float32).astype(jnp.bfloat16)

    choose = jnp.concatenate([chooser(0, 4), chooser(1, 5), chooser(2), chooser(3)], 0)
    inner_at = lax.broadcasted_iota(jnp.int32, (INNER, PT), 0).astype(jnp.float32)
    start_at = (lax.broadcasted_iota(jnp.int32, (outer, PT), 0) * INNER).astype(jnp.float32)
    total[...] = jnp.zeros_like(total)

    for s in range(seg_kept):
        seg = detector_bit * seg_kept + s
        own32[...] = own_ref[seg].astype(jnp.float32)
        other32[...] = other_ref[seg].astype(jnp.float32)
        own_r = own32[pl.ds(0, bands_half, stride=2), :]
        own_i = own32[pl.ds(1, bands_half, stride=2), :]
        other_r = other32[pl.ds(0, bands_half, stride=2), :]
        other_i = other32[pl.ds(1, bands_half, stride=2), :]
        cross[0] = own_r * other_r + own_i * other_i
        cross[1] = (own_r * other_i - own_i * other_r) * flip
        for b in range(bands_half):
            real = jnp.broadcast_to(cross[0, b : b + 1, :], (outer, width)) * mask
            imag = jnp.broadcast_to(cross[1, b : b + 1, :], (outer, width)) * mask
            high, low = split(jnp.concatenate([real, imag], 0))
            high_t, low_t = split(jnp.concatenate([imag, -real], 0))
            masked[b] = jnp.concatenate([high, high_t, low, low_t], 1)
        stacked = masked[...].reshape(bands_half * 2 * outer, 4 * width)
        left[...] = (
            jnp.dot(stacked, choose, preferred_element_type=jnp.float32)
            .astype(jnp.bfloat16)
            .reshape(bands_half, 2 * outer, LANES)
        )
        time_coord = ((tm_index * seg_count + seg).astype(jnp.float32) + 0.5 - segment_total / 2) / segment_total
        live = valid_ref[seg].astype(jnp.float32)

        def one_slot(slot, _):
            group = slot * TPB // per_group
            row = (2 * group + bin_half) * per_group + slot * TPB % per_group
            band = table_ref[0, row]
            lhs = left[band - bin_half * bands_half][:, : PARTS * INNER]
            turn = (band.astype(jnp.float32) + 0.5) / band_total * time_coord
            frequency = (band * width).astype(jnp.float32) + start_at
            for m in range(TPB):
                tile = table_ref[1, row + m]
                lag = jnp.concatenate([lags_ref[tile, c : c + 1, :] for c in range(per_tile)], 1)
                pace = jnp.concatenate([drift_ref[tile, c : c + 1, :] for c in range(per_tile)], 1)
                cosine, sine = near_turn(jnp.broadcast_to(lag, (INNER, PT)) * inner_at)
                cos_high, cos_low = split(cosine)
                sin_high, sin_low = split(sine)
                rhs = jnp.concatenate([cos_high, sin_high, cos_high, sin_high, cos_low, sin_low], 0)
                product = jnp.dot(lhs, rhs, preferred_element_type=jnp.float32)
                angle = jnp.broadcast_to(pace * turn, (outer, PT)) - frequency * jnp.broadcast_to(lag, (outer, PT))
                cosine, sine = any_turn(angle)
                terms = jnp.sum(cosine * product[:outer] - sine * product[outer:], axis=0, keepdims=True) * live
                for c in range(per_tile):
                    at = tile * per_tile + c
                    where = at // rows_dest, s, pl.ds(at % rows_dest, 1)
                    total[where] += terms[:, c * LANES : (c + 1) * LANES]
            return 0

        lax.fori_loop(0, slots, one_slot, 0)
        for n, data in enumerate((own32, other32)):
            power = jnp.sum(jnp.sum(data[...] * data[...], axis=0, keepdims=True), axis=1, keepdims=True)
            high = power.astype(jnp.bfloat16).astype(jnp.float32)
            for p, value in enumerate((high, power - high)):
                where = slice(None), s, pl.ds(rows_dest + 2 * n + p, 1)
                total[where] = jnp.broadcast_to(value.reshape(1, 1, 1), (total.shape[0], 1, LANES))
    out_ref[...] = total[...].astype(jnp.bfloat16)


def weights_of(power, fourier_bins):
    halves = power[..., 0::2, :] + power[..., 1::2, :]
    whole = halves.reshape(2, 2, *halves.shape[1:]).sum(1) / fourier_bins + 1e-06
    return 1.0 / (whole[..., 0, :] * whole[..., 1, :])


def sum_kernel(tm_count, rows_dest, fourier_bins, scale, got_ref, out_ref):
    seg_kept = got_ref.shape[1]
    total = jnp.zeros((rows_dest, LANES), jnp.float32)
    for k in range(2):
        for i in range(tm_count):
            for s in range(seg_kept):
                pair = [got_ref[(2 * k + h) * tm_count + i, s].astype(jnp.float32) for h in range(2)]
                both = pair[0] + pair[1]
                own = (both[rows_dest : rows_dest + 1] + both[rows_dest + 1 : rows_dest + 2]) / fourier_bins + 1e-06
                other = (both[rows_dest + 2 : rows_dest + 3] + both[rows_dest + 3 : rows_dest + 4]) / fourier_bins + 1e-06
                total = total + both[:rows_dest] * (1.0 / (own * other))
    out_ref[...] = total / scale


def shards(spectra, valid, lags, drift, block_table):
    det_count, tm_count = lax.axis_size("det"), lax.axis_size("tm")
    devices = det_count * tm_count
    own = spectra[0]
    seg_count, bands_half, _, width = own.shape
    seg_kept = seg_count // 2
    pixels = lags.shape[0]
    per_device = pixels // devices
    fourier_bins = 2 * bands_half * width
    scale = math.sqrt(seg_count * tm_count * width)
    direct = per_device % LANES == 0
    rows_dest = (per_device if direct else pixels) // LANES
    dests = devices if direct else 1
    rows = -(-(rows_dest + 4) // 8) * 8
    per_tile = PT // LANES

    own = own.reshape(seg_count, 2 * bands_half, width)
    other = lax.ppermute(own, "det", [(d, d ^ 2) for d in range(det_count)])
    place = jnp.stack([lax.axis_index("det"), lax.axis_index("tm")]).astype(jnp.int32)
    outgoing = pl.pallas_call(
        functools.partial(terms_kernel, tm_count, rows_dest, seg_kept),
        out_shape=jax.ShapeDtypeStruct((dests, seg_kept, rows, LANES), jnp.bfloat16),
        in_specs=[SMEM] * 3 + [VMEM] * 4,
        out_specs=VMEM,
        scratch_shapes=[
            pltpu.VMEM((2 * bands_half, width), jnp.float32),
            pltpu.VMEM((2 * bands_half, width), jnp.float32),
            pltpu.VMEM((2, bands_half, width), jnp.float32),
            pltpu.VMEM((bands_half, 2 * width // INNER, 4 * width), jnp.bfloat16),
            pltpu.VMEM((bands_half, 2 * width // INNER, LANES), jnp.bfloat16),
            pltpu.VMEM((dests, seg_kept, rows, LANES), jnp.float32),
        ],
        name="terms",
    )(place, valid, block_table.T, own, other, lags.reshape(-1, per_tile, LANES), drift.reshape(-1, per_tile, LANES))
    if direct:
        received = lax.all_to_all(outgoing, ("det", "tm"), 0, 0, tiled=True)
        result = pl.pallas_call(
            functools.partial(sum_kernel, tm_count, rows_dest, fourier_bins, scale),
            out_shape=jax.ShapeDtypeStruct((rows_dest, LANES), jnp.float32),
            in_specs=[VMEM],
            out_specs=VMEM,
            name="sum",
        )(received)
        return result.reshape(-1)
    maps = jnp.moveaxis(outgoing[0, :, :rows_dest].reshape(seg_kept, devices, per_device), 1, 0)
    powers = jnp.broadcast_to(outgoing[0, :, rows_dest : rows_dest + 4, 0], (devices, seg_kept, 4))
    sent = jnp.concatenate([maps, powers], 2)
    received = lax.all_to_all(sent, ("det", "tm"), 0, 0, tiled=True).astype(jnp.float32)
    received = received.reshape(det_count, tm_count, seg_kept, per_device + 4)
    weight = weights_of(received[..., per_device:, None], fourier_bins)[..., 0]
    both = received[..., :per_device].reshape(2, 2, tm_count, seg_kept, per_device).sum(1)
    return (both * weight[..., None]).sum((0, 1, 2)) / scale


def solution(mesh):
    placed = (P("det", "tm", None, None, None), P("tm"), P(), P(), P())
    return jax.shard_map(
        shards, mesh=mesh, in_specs=placed, out_specs=P(("det", "tm")), check_vma=False
    )
```

```python
import functools
import math

import jax
import jax.numpy as jnp
import numpy as np
from jax import lax
from jax.experimental import pallas as pl
from jax.experimental.pallas import tpu as pltpu
from jax.sharding import PartitionSpec as P

PT = 512
TPB = 2
LANES = 128
INNER = 16
PARTS = 6
UNROLLED = 16
GRANT = pltpu.CompilerParams(vmem_limit_bytes=8 << 20)

NEAR_COS = (0.9999999994443334, -19.739207715972064, 64.93905415215964, -85.41956519425082, 58.57456432893444)
NEAR_SIN = (6.283185306861161, -41.341701618023556, 81.60505457483515, -76.68452620857785, 41.10289536853278)
VMEM = pl.BlockSpec(memory_space=pltpu.VMEM)
HBM = pl.BlockSpec(memory_space=pltpu.HBM)


def fitted(function, limit, degree):
    nodes = (np.cos(np.pi * (np.arange(400) + 0.5) / 400) + 1) / 2
    powers = np.vander(nodes, degree + 1, increasing=True)
    coefficients = np.linalg.lstsq(powers, function(np.sqrt(nodes * limit)), rcond=None)[0]
    return tuple(float(c) for c in coefficients / limit ** np.arange(degree + 1))


FAR_COS = fitted(lambda r: np.cos(2 * np.pi * r), 0.25, 6)
FAR_SIN = fitted(lambda r: np.sin(2 * np.pi * r) / r, 0.25, 6)


def horner(coefficients, z):
    total = jnp.full_like(z, coefficients[-1])
    for c in coefficients[-2::-1]:
        total = total * z + c
    return total


def near_turn(x):
    z = x * x
    return horner(NEAR_COS, z), x * horner(NEAR_SIN, z)


def any_turn(x):
    r = x - jnp.floor(x + 0.5)
    z = r * r
    return horner(FAR_COS, z), r * horner(FAR_SIN, z)


def split(x):
    high = x.astype(jnp.bfloat16)
    return high, (x - high.astype(jnp.float32)).astype(jnp.bfloat16)


def block_of(slot, table_ref, tm_count, bin_half):
    per_group = table_ref.shape[1] // (2 * tm_count)
    first = slot * TPB
    return (2 * (first // per_group) + bin_half) * per_group + first % per_group


def over_slots(slots, one_slot):
    if slots <= UNROLLED:
        for slot in range(slots):
            one_slot(slot)
    else:
        lax.fori_loop(0, slots, lambda slot, _: (one_slot(slot), 0)[1], 0)


def inner_tables(tile, lags_ref, inner_at):
    lag = jnp.concatenate([lags_ref[tile, c : c + 1, :] for c in range(PT // LANES)], 1)
    cosine, sine = near_turn(jnp.broadcast_to(lag, inner_at.shape) * inner_at)
    cos_high, cos_low = split(cosine)
    sin_high, sin_low = split(sine)
    return lag, (cos_high, sin_high, cos_low, sin_low)


def outer_tables(tile, lag, drift_ref, turn, frequency, live):
    pace = jnp.concatenate([drift_ref[tile, c : c + 1, :] for c in range(PT // LANES)], 1)
    shape = frequency.shape
    cosine, sine = any_turn(jnp.broadcast_to(pace * turn, shape) - frequency * jnp.broadcast_to(lag, shape))
    return cosine * live, sine * live


def clock(valid_ref, tm_count, detector_bit, seg_kept):
    tm_index = lax.axis_index("tm")
    seg_count = valid_ref.shape[0]
    segment_total = seg_count * tm_count
    marks = []
    for s in range(seg_kept):
        seg = detector_bit * seg_kept + s
        time = ((tm_index * seg_count + seg).astype(jnp.float32) + 0.5 - segment_total / 2) / segment_total
        marks.append((valid_ref[seg].astype(jnp.float32), time))
    return marks


def fetch(sources, targets, sems):
    copies = [pltpu.make_async_copy(a, b, sems.at[n]) for n, (a, b) in enumerate(zip(sources, targets))]
    for copy in copies:
        copy.start()
    return copies


def start_rows(outer):
    return (lax.broadcasted_iota(jnp.int32, (outer, PT), 0) * INNER).astype(jnp.float32)


def inner_rows():
    return lax.broadcasted_iota(jnp.int32, (INNER, PT), 0).astype(jnp.float32)


def tables_kernel(
    tm_count, bands_half, width, seg_kept,
    valid_hbm, table_hbm, lags_hbm, drift_hbm,
    inner_ref, outer_ref,
    valid_ref, table_ref, lags_ref, drift_ref, sems,
):
    det_index = lax.axis_index("det")
    bin_half, detector_bit = det_index % 2, det_index // 2
    copies = fetch((valid_hbm, table_hbm, lags_hbm, drift_hbm), (valid_ref, table_ref, lags_ref, drift_ref), sems)
    inner_at, start_at = inner_rows(), start_rows(width // INNER)
    for copy in copies:
        copy.wait()
    marks = clock(valid_ref, tm_count, detector_bit, seg_kept)

    def one_slot(slot):
        row = block_of(slot, table_ref, tm_count, bin_half)
        band = table_ref[0, row]
        frequency = (band * width).astype(jnp.float32) + start_at
        share = (band.astype(jnp.float32) + 0.5) / (2 * bands_half)
        for m in range(TPB):
            tile = table_ref[1, row + m]
            at = slot * TPB + m
            lag, parts = inner_tables(tile, lags_ref, inner_at)
            inner_ref[at] = jnp.concatenate(parts, 0)
            for s, (live, time) in enumerate(marks):
                cosine, sine = outer_tables(tile, lag, drift_ref, share * time, frequency, live)
                outer_ref[at, s, 0] = cosine
                outer_ref[at, s, 1] = sine

    over_slots(inner_ref.shape[0] // TPB, one_slot)


def terms_kernel(tm_count, rows_dest, seg_kept, ready, *refs):
    if ready:
        table_hbm, inner_ref, outer_ref, own_ref, other_ref, out_ref, table_ref, sems, *scratch = refs
        copies = fetch((table_hbm,), (table_ref,), sems)
    else:
        valid_hbm, table_hbm, lags_hbm, drift_hbm, own_ref, other_ref, out_ref, *scratch = refs
        valid_ref, table_ref, lags_ref, drift_ref, sems, *scratch = scratch
        copies = fetch((valid_hbm, table_hbm, lags_hbm, drift_hbm), (valid_ref, table_ref, lags_ref, drift_ref), sems)
    own32, other32, cross, masked, left, total = scratch
    det_index = lax.axis_index("det")
    bin_half, detector_bit = det_index % 2, det_index // 2
    bands_half = own_ref.shape[1] // 2
    width = own_ref.shape[2]
    outer = width // INNER
    per_tile = PT // LANES
    flip = jnp.where(detector_bit == 0, 1.0, -1.0).astype(jnp.float32)
    outer_at = lax.broadcasted_iota(jnp.int32, (outer, width), 0)
    lane_at = lax.broadcasted_iota(jnp.int32, (outer, width), 1)
    mask = (lane_at // INNER == outer_at).astype(jnp.float32)
    from_lane = lax.broadcasted_iota(jnp.int32, (width, LANES), 0) % INNER
    to_lane = lax.broadcasted_iota(jnp.int32, (width, LANES), 1)
    same = from_lane == to_lane % INNER
    part = to_lane // INNER

    def chooser(*parts):
        chosen = part == parts[0]
        for p in parts[1:]:
            chosen = chosen | (part == p)
        return (same & chosen).astype(jnp.float32).astype(jnp.bfloat16)

    choose = jnp.concatenate([chooser(0, 4), chooser(1, 5), chooser(2), chooser(3)], 0)
    total[...] = jnp.zeros_like(total)

    for s in range(seg_kept):
        seg = detector_bit * seg_kept + s
        own32[...] = own_ref[seg].astype(jnp.float32)
        other32[...] = other_ref[seg].astype(jnp.float32)
        own_r = own32[pl.ds(0, bands_half, stride=2), :]
        own_i = own32[pl.ds(1, bands_half, stride=2), :]
        other_r = other32[pl.ds(0, bands_half, stride=2), :]
        other_i = other32[pl.ds(1, bands_half, stride=2), :]
        cross[0] = own_r * other_r + own_i * other_i
        cross[1] = (own_r * other_i - own_i * other_r) * flip
        for b in range(bands_half):
            real = jnp.broadcast_to(cross[0, b : b + 1, :], (outer, width)) * mask
            imag = jnp.broadcast_to(cross[1, b : b + 1, :], (outer, width)) * mask
            high, low = split(jnp.concatenate([real, imag], 0))
            high_t, low_t = split(jnp.concatenate([imag, -real], 0))
            masked[b] = jnp.concatenate([high, high_t, low, low_t], 1)
        stacked = masked[...].reshape(bands_half * 2 * outer, 4 * width)
        left[...] = (
            jnp.dot(stacked, choose, preferred_element_type=jnp.float32)
            .astype(jnp.bfloat16)
            .reshape(bands_half, 2 * outer, LANES)
        )
        if s == 0:
            for copy in copies:
                copy.wait()
        if not ready:
            inner_at, start_at = inner_rows(), start_rows(outer)
            live, time = clock(valid_ref, tm_count, detector_bit, seg_kept)[s]

        def one_slot(slot):
            row = block_of(slot, table_ref, tm_count, bin_half)
            band = table_ref[0, row]
            lhs = left[band - bin_half * bands_half][:, : PARTS * INNER]
            for m in range(TPB):
                at = slot * TPB + m
                tile = table_ref[1, row + m]
                if ready:
                    table = inner_ref[at]
                    cosine, sine = outer_ref[at, s, 0], outer_ref[at, s, 1]
                else:
                    lag, parts = inner_tables(tile, lags_ref, inner_at)
                    table = jnp.concatenate(parts, 0)
                    turn = (band.astype(jnp.float32) + 0.5) / (2 * bands_half) * time
                    frequency = (band * width).astype(jnp.float32) + start_at
                    cosine, sine = outer_tables(tile, lag, drift_ref, turn, frequency, live)
                rhs = jnp.concatenate([table[: 2 * INNER], table], 0)
                product = jnp.dot(lhs, rhs, preferred_element_type=jnp.float32)
                terms = jnp.sum(cosine * product[:outer] - sine * product[outer:], axis=0, keepdims=True)
                for c in range(per_tile):
                    piece = tile * per_tile + c
                    where = piece // rows_dest, s, pl.ds(piece % rows_dest, 1)
                    total[where] += terms[:, c * LANES : (c + 1) * LANES]

        over_slots(table_ref.shape[1] // 2 // TPB, one_slot)
        for n, data in enumerate((own32, other32)):
            power = jnp.sum(jnp.sum(data[...] * data[...], axis=0, keepdims=True), axis=1, keepdims=True)
            high = power.astype(jnp.bfloat16).astype(jnp.float32)
            for p, value in enumerate((high, power - high)):
                where = slice(None), s, pl.ds(rows_dest + 2 * n + p, 1)
                total[where] = jnp.broadcast_to(value.reshape(1, 1, 1), (total.shape[0], 1, LANES))
    out_ref[...] = total[...].astype(jnp.bfloat16)


def weights_of(power, fourier_bins):
    halves = power[..., 0::2, :] + power[..., 1::2, :]
    whole = halves.reshape(2, 2, *halves.shape[1:]).sum(1) / fourier_bins + 1e-06
    return 1.0 / (whole[..., 0, :] * whole[..., 1, :])


def sum_kernel(tm_count, rows_dest, fourier_bins, scale, got_ref, out_ref):
    seg_kept = got_ref.shape[1]
    total = jnp.zeros((rows_dest, LANES), jnp.float32)
    for k in range(2):
        for i in range(tm_count):
            for s in range(seg_kept):
                pair = [got_ref[(2 * k + h) * tm_count + i, s].astype(jnp.float32) for h in range(2)]
                both = pair[0] + pair[1]
                own = (both[rows_dest : rows_dest + 1] + both[rows_dest + 1 : rows_dest + 2]) / fourier_bins + 1e-06
                other = (both[rows_dest + 2 : rows_dest + 3] + both[rows_dest + 3 : rows_dest + 4]) / fourier_bins + 1e-06
                total = total + both[:rows_dest] * (1.0 / (own * other))
    out_ref[...] = total / scale


def shards(spectra, valid, lags, drift, block_table):
    det_count, tm_count = lax.axis_size("det"), lax.axis_size("tm")
    devices = det_count * tm_count
    own = spectra[0]
    seg_count, bands_half, _, width = own.shape
    seg_kept = seg_count // 2
    pixels = lags.shape[0]
    per_device = pixels // devices
    fourier_bins = 2 * bands_half * width
    scale = math.sqrt(seg_count * tm_count * width)
    direct = per_device % LANES == 0
    rows_dest = (per_device if direct else pixels) // LANES
    dests = devices if direct else 1
    rows = -(-(rows_dest + 4) // 8) * 8
    per_tile = PT // LANES

    blocks = block_table.shape[0] // 2
    outer = width // INNER
    own = own.reshape(seg_count, 2 * bands_half, width)
    other = lax.ppermute(own, "det", [(d, d ^ 2) for d in range(det_count)])
    table = block_table.T
    lags, drift = (x.reshape(-1, per_tile, LANES) for x in (lags, drift))
    settings = tuple(pltpu.with_memory_space_constraint(x, pltpu.HBM) for x in (valid, table, lags, drift))
    held = [pltpu.SMEM(valid.shape, jnp.int32), pltpu.SMEM(table.shape, jnp.int32)]
    held += [pltpu.VMEM(lags.shape, jnp.float32), pltpu.VMEM(drift.shape, jnp.float32)]
    held += [pltpu.SemaphoreType.DMA((len(settings),))]
    tables = [
        jax.ShapeDtypeStruct((blocks, 4 * INNER, PT), jnp.bfloat16),
        jax.ShapeDtypeStruct((blocks, seg_kept, 2, outer, PT), jnp.float32),
    ]
    ready = blocks <= 4 * UNROLLED
    if ready:
        made = pl.pallas_call(
            functools.partial(tables_kernel, tm_count, bands_half, width, seg_kept),
            out_shape=tables,
            in_specs=[HBM] * 4,
            out_specs=[VMEM] * 2,
            scratch_shapes=held,
            compiler_params=GRANT,
            cost_estimate=pl.CostEstimate(flops=10**9, bytes_accessed=10**6, transcendentals=0),
            name="tables",
        )(*settings)
        settings = (table, *made)
        held = [pltpu.SMEM(table.shape, jnp.int32), pltpu.SemaphoreType.DMA((1,))]
    outgoing = pl.pallas_call(
        functools.partial(terms_kernel, tm_count, rows_dest, seg_kept, ready),
        out_shape=jax.ShapeDtypeStruct((dests, seg_kept, rows, LANES), jnp.bfloat16),
        in_specs=([HBM] + [VMEM] * 2 if ready else [HBM] * 4) + [VMEM] * 2,
        out_specs=VMEM,
        scratch_shapes=held
        + [
            pltpu.VMEM((2 * bands_half, width), jnp.float32),
            pltpu.VMEM((2 * bands_half, width), jnp.float32),
            pltpu.VMEM((2, bands_half, width), jnp.float32),
            pltpu.VMEM((bands_half, 2 * outer, 4 * width), jnp.bfloat16),
            pltpu.VMEM((bands_half, 2 * outer, LANES), jnp.bfloat16),
            pltpu.VMEM((dests, seg_kept, rows, LANES), jnp.float32),
        ],
        compiler_params=GRANT,
        name="terms",
    )(*settings, own, other)
    if direct:
        received = lax.all_to_all(outgoing, ("det", "tm"), 0, 0, tiled=True)
        result = pl.pallas_call(
            functools.partial(sum_kernel, tm_count, rows_dest, fourier_bins, scale),
            out_shape=jax.ShapeDtypeStruct((rows_dest, LANES), jnp.float32),
            in_specs=[VMEM],
            out_specs=VMEM,
            compiler_params=GRANT,
            name="sum",
        )(received)
        return result.reshape(-1)
    maps = jnp.moveaxis(outgoing[0, :, :rows_dest].reshape(seg_kept, devices, per_device), 1, 0)
    powers = jnp.broadcast_to(outgoing[0, :, rows_dest : rows_dest + 4, 0], (devices, seg_kept, 4))
    sent = jnp.concatenate([maps, powers], 2)
    received = lax.all_to_all(sent, ("det", "tm"), 0, 0, tiled=True).astype(jnp.float32)
    received = received.reshape(det_count, tm_count, seg_kept, per_device + 4)
    weight = weights_of(received[..., per_device:, None], fourier_bins)[..., 0]
    both = received[..., :per_device].reshape(2, 2, tm_count, seg_kept, per_device).sum(1)
    return (both * weight[..., None]).sum((0, 1, 2)) / scale


def solution(mesh):
    placed = (P("det", "tm", None, None, None), P("tm"), P(), P(), P())
    return jax.shard_map(
        shards, mesh=mesh, in_specs=placed, out_specs=P(("det", "tm")), check_vma=False
    )
```

```python
import functools
import math

import jax
import jax.numpy as jnp
import numpy as np
from jax import lax
from jax.experimental import pallas as pl
from jax.experimental.pallas import tpu as pltpu
from jax.sharding import PartitionSpec as P

PT = 512
TPB = 2
LANES = 128
INNER = 16
PARTS = 6
UNROLLED = 16
GRANT = pltpu.CompilerParams(vmem_limit_bytes=8 << 20)

NEAR_COS = (0.9999999994443334, -19.739207715972064, 64.93905415215964, -85.41956519425082, 58.57456432893444)
NEAR_SIN = (6.283185306861161, -41.341701618023556, 81.60505457483515, -76.68452620857785, 41.10289536853278)
VMEM = pl.BlockSpec(memory_space=pltpu.VMEM)
HBM = pl.BlockSpec(memory_space=pltpu.HBM)


def fitted(function, limit, degree):
    nodes = (np.cos(np.pi * (np.arange(400) + 0.5) / 400) + 1) / 2
    powers = np.vander(nodes, degree + 1, increasing=True)
    coefficients = np.linalg.lstsq(powers, function(np.sqrt(nodes * limit)), rcond=None)[0]
    return tuple(float(c) for c in coefficients / limit ** np.arange(degree + 1))


FAR_COS = fitted(lambda r: np.cos(2 * np.pi * r), 0.25, 6)
FAR_SIN = fitted(lambda r: np.sin(2 * np.pi * r) / r, 0.25, 6)


def horner(coefficients, z):
    total = jnp.full_like(z, coefficients[-1])
    for c in coefficients[-2::-1]:
        total = total * z + c
    return total


def near_turn(x):
    z = x * x
    return horner(NEAR_COS, z), x * horner(NEAR_SIN, z)


def any_turn(x):
    r = x - jnp.floor(x + 0.5)
    z = r * r
    return horner(FAR_COS, z), r * horner(FAR_SIN, z)


def split(x):
    high = x.astype(jnp.bfloat16)
    return high, (x - high.astype(jnp.float32)).astype(jnp.bfloat16)


def block_of(slot, table_ref, tm_count, bin_half):
    per_group = table_ref.shape[1] // (2 * tm_count)
    first = slot * TPB
    return (2 * (first // per_group) + bin_half) * per_group + first % per_group


def over_slots(slots, one_slot):
    if slots <= UNROLLED:
        for slot in range(slots):
            one_slot(slot)
    else:
        lax.fori_loop(0, slots, lambda slot, _: (one_slot(slot), 0)[1], 0)


def inner_tables(tile, lags_ref, inner_at):
    lag = jnp.concatenate([lags_ref[tile, c : c + 1, :] for c in range(PT // LANES)], 1)
    cosine, sine = near_turn(jnp.broadcast_to(lag, inner_at.shape) * inner_at)
    cos_high, cos_low = split(cosine)
    sin_high, sin_low = split(sine)
    return lag, (cos_high, sin_high, cos_low, sin_low)


def outer_tables(tile, lag, drift_ref, turn, frequency, live):
    pace = jnp.concatenate([drift_ref[tile, c : c + 1, :] for c in range(PT // LANES)], 1)
    shape = frequency.shape
    cosine, sine = any_turn(jnp.broadcast_to(pace * turn, shape) - frequency * jnp.broadcast_to(lag, shape))
    return cosine * live, sine * live


def clock(valid_ref, tm_count, detector_bit, seg_kept):
    tm_index = lax.axis_index("tm")
    seg_count = valid_ref.shape[0]
    segment_total = seg_count * tm_count
    marks = []
    for s in range(seg_kept):
        seg = detector_bit * seg_kept + s
        time = ((tm_index * seg_count + seg).astype(jnp.float32) + 0.5 - segment_total / 2) / segment_total
        marks.append((valid_ref[seg].astype(jnp.float32), time))
    return marks


def fetch(sources, targets, sems):
    copies = [pltpu.make_async_copy(a, b, sems.at[n]) for n, (a, b) in enumerate(zip(sources, targets))]
    for copy in copies:
        copy.start()
    return copies


def start_rows(outer):
    return (lax.broadcasted_iota(jnp.int32, (outer, PT), 0) * INNER).astype(jnp.float32)


def inner_rows():
    return lax.broadcasted_iota(jnp.int32, (INNER, PT), 0).astype(jnp.float32)


def spreading(outer, width):
    lane_at = lax.broadcasted_iota(jnp.int32, (outer, width), 1)
    mask = (lane_at // INNER == lax.broadcasted_iota(jnp.int32, (outer, width), 0)).astype(jnp.float32)
    from_lane = lax.broadcasted_iota(jnp.int32, (width, LANES), 0)
    to_lane = lax.broadcasted_iota(jnp.int32, (width, LANES), 1)
    choose = (from_lane % INNER == to_lane % INNER).astype(jnp.float32).astype(jnp.bfloat16)
    return mask, choose


def spread(rows_ref, band_of, masked, outer, width):
    mask, choose = spreading(outer, width)

    def one_slot(slot):
        row = 2 * band_of(slot)
        pair = [jnp.broadcast_to(rows_ref[pl.ds(row + c, 1), :], (outer, width)) * mask for c in range(2)]
        masked[slot] = jnp.concatenate(pair, 0).astype(jnp.bfloat16)

    slots = masked.shape[0]
    over_slots(slots, one_slot)
    stacked = masked[...].reshape(slots * 2 * outer, width)
    return jnp.dot(stacked, choose, preferred_element_type=jnp.float32).reshape(slots, 2 * outer, LANES)


def mix_own(rows_ref, band_of, masked, mixed_ref, s, flip, outer, width):
    wide = spread(rows_ref, band_of, masked, outer, width)
    real, imag = wide[:, :outer], wide[:, outer:]
    even = lax.broadcasted_iota(jnp.int32, real.shape, 2) // INNER % 2 == 0
    mixed_ref[s, 0] = jnp.where(even, real, -flip * imag)
    mixed_ref[s, 1] = jnp.where(even, imag, flip * real)
    mixed_ref[s, 2] = jnp.where(even, -flip * imag, -real)
    mixed_ref[s, 3] = jnp.where(even, flip * real, -imag)


def power_rows(rows):
    power = jnp.sum(jnp.sum(rows * rows, axis=0, keepdims=True), axis=1, keepdims=True)
    high = power.astype(jnp.bfloat16).astype(jnp.float32)
    return jnp.concatenate([jnp.broadcast_to(x, (1, LANES)) for x in (high, power - high)], 0)


def tables_kernel(
    tm_count, bands_half, width, seg_kept,
    valid_hbm, table_hbm, lags_hbm, drift_hbm, own_ref,
    inner_ref, outer_ref, mixed_ref, power_ref,
    valid_ref, table_ref, lags_ref, drift_ref, sems, rows32, masked,
):
    det_index = lax.axis_index("det")
    bin_half, detector_bit = det_index % 2, det_index // 2
    copies = fetch((valid_hbm, table_hbm, lags_hbm, drift_hbm), (valid_ref, table_ref, lags_ref, drift_ref), sems)
    outer = width // INNER
    inner_at, start_at = inner_rows(), start_rows(outer)
    flip = jnp.where(detector_bit == 0, 1.0, -1.0).astype(jnp.float32)
    copies[1].wait()

    def band_of(slot):
        return table_ref[0, block_of(slot, table_ref, tm_count, bin_half)] - bin_half * bands_half

    for s in range(seg_kept):
        rows32[...] = own_ref[detector_bit * seg_kept + s].astype(jnp.float32)
        power_ref[s] = power_rows(rows32[...])
        mix_own(rows32, band_of, masked, mixed_ref, s, flip, outer, width)
    for n in (0, 2, 3):
        copies[n].wait()
    marks = clock(valid_ref, tm_count, detector_bit, seg_kept)

    def one_slot(slot):
        row = block_of(slot, table_ref, tm_count, bin_half)
        band = table_ref[0, row]
        frequency = (band * width).astype(jnp.float32) + start_at
        share = (band.astype(jnp.float32) + 0.5) / (2 * bands_half)
        for m in range(TPB):
            tile = table_ref[1, row + m]
            at = slot * TPB + m
            lag, parts = inner_tables(tile, lags_ref, inner_at)
            inner_ref[at] = jnp.concatenate(parts, 0)
            for s, (live, time) in enumerate(marks):
                cosine, sine = outer_tables(tile, lag, drift_ref, share * time, frequency, live)
                outer_ref[at, s, 0] = cosine
                outer_ref[at, s, 1] = sine

    over_slots(inner_ref.shape[0] // TPB, one_slot)


def terms_kernel(tm_count, dests, rows_dest, seg_kept, ready, *refs):
    if ready:
        table_hbm, inner_ref, outer_ref, mixed_ref, power_ref, other_ref, out_ref, table_ref, sems, *scratch = refs
        copies = fetch((table_hbm,), (table_ref,), sems)
    else:
        valid_hbm, table_hbm, lags_hbm, drift_hbm, own_ref, other_ref, out_ref, *scratch = refs
        valid_ref, table_ref, lags_ref, drift_ref, sems, mixed_ref, *scratch = scratch
        copies = fetch((valid_hbm, table_hbm, lags_hbm, drift_hbm), (valid_ref, table_ref, lags_ref, drift_ref), sems)
    rows32, masked, left, total = scratch
    det_index = lax.axis_index("det")
    bin_half, detector_bit = det_index % 2, det_index // 2
    bands_half = other_ref.shape[1] // 2
    width = other_ref.shape[2]
    outer = width // INNER
    per_tile = PT // LANES
    slots = masked.shape[0]
    flip = jnp.where(detector_bit == 0, 1.0, -1.0).astype(jnp.float32)
    part = lax.broadcasted_iota(jnp.int32, (slots, outer, LANES), 2) // INNER
    total[...] = jnp.zeros_like(total)

    def band_of(slot):
        return table_ref[0, block_of(slot, table_ref, tm_count, bin_half)] - bin_half * bands_half

    for s in range(seg_kept):
        seg = detector_bit * seg_kept + s
        rows32[...] = other_ref[seg].astype(jnp.float32)
        powers = [power_ref[s] if ready else power_rows(own_ref[seg].astype(jnp.float32)), power_rows(rows32[...])]
        if s == 0:
            for copy in copies:
                copy.wait()
        wide = spread(rows32, band_of, masked, outer, width)
        if not ready:
            rows32[...] = own_ref[seg].astype(jnp.float32)
            mix_own(rows32, band_of, masked, mixed_ref, s, flip, outer, width)
            inner_at, start_at = inner_rows(), start_rows(outer)
            live, time = clock(valid_ref, tm_count, detector_bit, seg_kept)[s]
        real, imag = wide[:, :outer], wide[:, outer:]
        for n in range(2):
            value = mixed_ref[s, 2 * n] * real + mixed_ref[s, 2 * n + 1] * imag
            high = value.astype(jnp.bfloat16).astype(jnp.float32)
            parts = jnp.where((part == 2) | (part == 3), value - high, high)
            left[:, n * outer : (n + 1) * outer, :] = parts

        def one_slot(slot):
            row = block_of(slot, table_ref, tm_count, bin_half)
            lhs = left[slot][:, : PARTS * INNER].astype(jnp.bfloat16)
            for m in range(TPB):
                at = slot * TPB + m
                tile = table_ref[1, row + m]
                if ready:
                    table = inner_ref[at]
                    cosine, sine = outer_ref[at, s, 0], outer_ref[at, s, 1]
                else:
                    band = table_ref[0, row]
                    lag, parts = inner_tables(tile, lags_ref, inner_at)
                    table = jnp.concatenate(parts, 0)
                    turn = (band.astype(jnp.float32) + 0.5) / (2 * bands_half) * time
                    frequency = (band * width).astype(jnp.float32) + start_at
                    cosine, sine = outer_tables(tile, lag, drift_ref, turn, frequency, live)
                rhs = jnp.concatenate([table[: 2 * INNER], table], 0)
                product = jnp.dot(lhs, rhs, preferred_element_type=jnp.float32)
                terms = jnp.sum(cosine * product[:outer] - sine * product[outer:], axis=0, keepdims=True)
                total[s, tile] += jnp.concatenate([terms[:, c * LANES : (c + 1) * LANES] for c in range(per_tile)], 0)

        over_slots(slots, one_slot)
        tiles = rows_dest // per_tile
        powers = jnp.concatenate(powers, 0)
        for d in range(dests):
            piece = total[s, d * tiles : (d + 1) * tiles].reshape(rows_dest, LANES)
            out_ref[d, s] = jnp.concatenate([piece, powers], 0).astype(jnp.bfloat16)


def weights_of(power, fourier_bins):
    halves = power[..., 0::2, :] + power[..., 1::2, :]
    whole = halves.reshape(2, 2, *halves.shape[1:]).sum(1) / fourier_bins + 1e-06
    return 1.0 / (whole[..., 0, :] * whole[..., 1, :])


def sum_kernel(tm_count, rows_dest, fourier_bins, scale, got_ref, out_ref):
    seg_kept = got_ref.shape[1]
    total = jnp.zeros((rows_dest, LANES), jnp.float32)
    for k in range(2):
        for i in range(tm_count):
            for s in range(seg_kept):
                pair = [got_ref[(2 * k + h) * tm_count + i, s].astype(jnp.float32) for h in range(2)]
                both = pair[0] + pair[1]
                own = (both[rows_dest : rows_dest + 1] + both[rows_dest + 1 : rows_dest + 2]) / fourier_bins + 1e-06
                other = (both[rows_dest + 2 : rows_dest + 3] + both[rows_dest + 3 : rows_dest + 4]) / fourier_bins + 1e-06
                total = total + both[:rows_dest] * (1.0 / (own * other))
    out_ref[...] = total / scale


def shards(spectra, valid, lags, drift, block_table):
    det_count, tm_count = lax.axis_size("det"), lax.axis_size("tm")
    devices = det_count * tm_count
    own = spectra[0]
    seg_count, bands_half, _, width = own.shape
    seg_kept = seg_count // 2
    pixels = lags.shape[0]
    per_device = pixels // devices
    fourier_bins = 2 * bands_half * width
    scale = math.sqrt(seg_count * tm_count * width)
    direct = per_device % PT == 0
    rows_dest = (per_device if direct else pixels) // LANES
    dests = devices if direct else 1
    rows = rows_dest + 4
    per_tile = PT // LANES
    blocks = block_table.shape[0] // 2
    slots = blocks // TPB
    outer = width // INNER

    own = own.reshape(seg_count, 2 * bands_half, width)
    other = lax.ppermute(own, "det", [(d, d ^ 2) for d in range(det_count)])
    table = block_table.T
    lags, drift = (x.reshape(-1, per_tile, LANES) for x in (lags, drift))
    settings = tuple(pltpu.with_memory_space_constraint(x, pltpu.HBM) for x in (valid, table, lags, drift))
    held = [pltpu.SMEM(valid.shape, jnp.int32), pltpu.SMEM(table.shape, jnp.int32)]
    held += [pltpu.VMEM(lags.shape, jnp.float32), pltpu.VMEM(drift.shape, jnp.float32)]
    held += [pltpu.SemaphoreType.DMA((len(settings),))]
    work = [pltpu.VMEM(own.shape[1:], jnp.float32), pltpu.VMEM((slots, 2 * outer, width), jnp.bfloat16)]
    mixed = jax.ShapeDtypeStruct((seg_kept, 4, slots, outer, LANES), jnp.float32)
    ready = slots <= UNROLLED
    if ready:
        made = pl.pallas_call(
            functools.partial(tables_kernel, tm_count, bands_half, width, seg_kept),
            out_shape=[
                jax.ShapeDtypeStruct((blocks, 4 * INNER, PT), jnp.bfloat16),
                jax.ShapeDtypeStruct((blocks, seg_kept, 2, outer, PT), jnp.float32),
                mixed,
                jax.ShapeDtypeStruct((seg_kept, 2, LANES), jnp.float32),
            ],
            in_specs=[HBM] * 4 + [VMEM],
            out_specs=[VMEM] * 4,
            scratch_shapes=held + work,
            compiler_params=GRANT,
            cost_estimate=pl.CostEstimate(flops=10**9, bytes_accessed=10**6, transcendentals=0),
            name="tables",
        )(*settings, own)
        settings = (table, *made)
        held = [pltpu.SMEM(table.shape, jnp.int32), pltpu.SemaphoreType.DMA((1,))]
    else:
        settings = (*settings, own)
        held += [pltpu.VMEM(mixed.shape, mixed.dtype)]
    outgoing = pl.pallas_call(
        functools.partial(terms_kernel, tm_count, dests, rows_dest, seg_kept, ready),
        out_shape=jax.ShapeDtypeStruct((dests, seg_kept, rows, LANES), jnp.bfloat16),
        in_specs=([HBM] + [VMEM] * 4 if ready else [HBM] * 4 + [VMEM]) + [VMEM],
        out_specs=VMEM,
        scratch_shapes=[
            *held,
            *work,
            pltpu.VMEM((slots, 2 * outer, LANES), jnp.float32),
            pltpu.VMEM((seg_kept, pixels // PT, per_tile, LANES), jnp.float32),
        ],
        compiler_params=GRANT if ready else None,
        name="terms",
    )(*settings, other)
    if direct:
        received = lax.all_to_all(outgoing, ("det", "tm"), 0, 0, tiled=True)
        result = pl.pallas_call(
            functools.partial(sum_kernel, tm_count, rows_dest, fourier_bins, scale),
            out_shape=jax.ShapeDtypeStruct((rows_dest, LANES), jnp.float32),
            in_specs=[VMEM],
            out_specs=VMEM,
            compiler_params=GRANT,
            name="sum",
        )(received)
        return result.reshape(-1)
    maps = jnp.moveaxis(outgoing[0, :, :rows_dest].reshape(seg_kept, devices, per_device), 1, 0)
    powers = jnp.broadcast_to(outgoing[0, :, rows_dest : rows_dest + 4, 0], (devices, seg_kept, 4))
    sent = jnp.concatenate([maps, powers], 2)
    received = lax.all_to_all(sent, ("det", "tm"), 0, 0, tiled=True).astype(jnp.float32)
    received = received.reshape(det_count, tm_count, seg_kept, per_device + 4)
    weight = weights_of(received[..., per_device:, None], fourier_bins)[..., 0]
    both = received[..., :per_device].reshape(2, 2, tm_count, seg_kept, per_device).sum(1)
    return (both * weight[..., None]).sum((0, 1, 2)) / scale


def solution(mesh):
    placed = (P("det", "tm", None, None, None), P("tm"), P(), P(), P())
    return jax.shard_map(
        shards, mesh=mesh, in_specs=placed, out_specs=P(("det", "tm")), check_vma=False
    )
```

```python
import functools
import math

import jax
import jax.numpy as jnp
import numpy as np
from jax import lax
from jax.experimental import pallas as pl
from jax.experimental.pallas import tpu as pltpu
from jax.sharding import PartitionSpec as P

PT = 512
TPB = 2
LANES = 128
INNER = 16
PARTS = 6
UNROLLED = 16
GRANT = pltpu.CompilerParams(vmem_limit_bytes=8 << 20)

NEAR_COS = (0.9999999994443334, -19.739207715972064, 64.93905415215964, -85.41956519425082, 58.57456432893444)
NEAR_SIN = (6.283185306861161, -41.341701618023556, 81.60505457483515, -76.68452620857785, 41.10289536853278)
VMEM = pl.BlockSpec(memory_space=pltpu.VMEM)
HBM = pl.BlockSpec(memory_space=pltpu.HBM)


def fitted(function, limit, degree):
    nodes = (np.cos(np.pi * (np.arange(400) + 0.5) / 400) + 1) / 2
    powers = np.vander(nodes, degree + 1, increasing=True)
    coefficients = np.linalg.lstsq(powers, function(np.sqrt(nodes * limit)), rcond=None)[0]
    return tuple(float(c) for c in coefficients / limit ** np.arange(degree + 1))


FAR_COS = fitted(lambda r: np.cos(2 * np.pi * r), 0.25, 6)
FAR_SIN = fitted(lambda r: np.sin(2 * np.pi * r) / r, 0.25, 6)


def horner(coefficients, z):
    total = jnp.full_like(z, coefficients[-1])
    for c in coefficients[-2::-1]:
        total = total * z + c
    return total


def near_turn(x):
    z = x * x
    return horner(NEAR_COS, z), x * horner(NEAR_SIN, z)


def any_turn(x):
    r = x - jnp.floor(x + 0.5)
    z = r * r
    return horner(FAR_COS, z), r * horner(FAR_SIN, z)


def split(x):
    high = x.astype(jnp.bfloat16)
    return high, (x - high.astype(jnp.float32)).astype(jnp.bfloat16)


def block_of(slot, table_ref, tm_count, bin_half):
    per_group = table_ref.shape[1] // (2 * tm_count)
    first = slot * TPB
    return (2 * (first // per_group) + bin_half) * per_group + first % per_group


def over_slots(slots, one_slot):
    if slots <= UNROLLED:
        for slot in range(slots):
            one_slot(slot)
    else:
        lax.fori_loop(0, slots, lambda slot, _: (one_slot(slot), 0)[1], 0)


def inner_tables(tile, lags_ref, inner_at):
    lag = jnp.concatenate([lags_ref[tile, c : c + 1, :] for c in range(PT // LANES)], 1)
    cosine, sine = near_turn(jnp.broadcast_to(lag, inner_at.shape) * inner_at)
    cos_high, cos_low = split(cosine)
    sin_high, sin_low = split(sine)
    return lag, (cos_high, sin_high, cos_low, sin_low)


def outer_tables(tile, lag, drift_ref, turn, frequency, live):
    pace = jnp.concatenate([drift_ref[tile, c : c + 1, :] for c in range(PT // LANES)], 1)
    shape = frequency.shape
    cosine, sine = any_turn(jnp.broadcast_to(pace * turn, shape) - frequency * jnp.broadcast_to(lag, shape))
    return cosine * live, sine * live


def clock(valid_ref, tm_count, detector_bit, seg_kept):
    tm_index = lax.axis_index("tm")
    seg_count = valid_ref.shape[0]
    segment_total = seg_count * tm_count
    marks = []
    for s in range(seg_kept):
        seg = detector_bit * seg_kept + s
        time = ((tm_index * seg_count + seg).astype(jnp.float32) + 0.5 - segment_total / 2) / segment_total
        marks.append((valid_ref[seg].astype(jnp.float32), time))
    return marks


def fetch(sources, targets, sems):
    copies = [pltpu.make_async_copy(a, b, sems.at[n]) for n, (a, b) in enumerate(zip(sources, targets))]
    for copy in copies:
        copy.start()
    return copies


def start_rows(outer):
    return (lax.broadcasted_iota(jnp.int32, (outer, PT), 0) * INNER).astype(jnp.float32)


def inner_rows():
    return lax.broadcasted_iota(jnp.int32, (INNER, PT), 0).astype(jnp.float32)


def spreading(outer, width):
    lane_at = lax.broadcasted_iota(jnp.int32, (outer, width), 1)
    mask = (lane_at // INNER == lax.broadcasted_iota(jnp.int32, (outer, width), 0)).astype(jnp.float32)
    from_lane = lax.broadcasted_iota(jnp.int32, (width, LANES), 0)
    to_lane = lax.broadcasted_iota(jnp.int32, (width, LANES), 1)
    choose = (from_lane % INNER == to_lane % INNER).astype(jnp.float32).astype(jnp.bfloat16)
    return mask, choose


def spread(rows_ref, band_of, masked, outer, width):
    mask, choose = spreading(outer, width)

    def one_slot(slot):
        row = 2 * band_of(slot)
        pair = [jnp.broadcast_to(rows_ref[pl.ds(row + c, 1), :], (outer, width)) * mask for c in range(2)]
        masked[slot] = jnp.concatenate(pair, 0).astype(jnp.bfloat16)

    slots = masked.shape[0]
    over_slots(slots, one_slot)
    stacked = masked[...].reshape(slots * 2 * outer, width)
    return jnp.dot(stacked, choose, preferred_element_type=jnp.float32).reshape(slots, 2 * outer, LANES)


def mix_own(rows_ref, band_of, masked, mixed_ref, s, flip, outer, width):
    wide = spread(rows_ref, band_of, masked, outer, width)
    real, imag = wide[:, :outer], wide[:, outer:]
    even = lax.broadcasted_iota(jnp.int32, real.shape, 2) // INNER % 2 == 0
    mixed_ref[s, 0] = jnp.where(even, real, -flip * imag)
    mixed_ref[s, 1] = jnp.where(even, imag, flip * real)
    mixed_ref[s, 2] = jnp.where(even, -flip * imag, -real)
    mixed_ref[s, 3] = jnp.where(even, flip * real, -imag)


def power_rows(rows):
    power = jnp.sum(jnp.sum(rows * rows, axis=0, keepdims=True), axis=1, keepdims=True)
    high = power.astype(jnp.bfloat16).astype(jnp.float32)
    return jnp.concatenate([jnp.broadcast_to(x, (1, LANES)) for x in (high, power - high)], 0)


def tables_kernel(
    tm_count, bands_half, width, seg_kept,
    valid_hbm, table_hbm, lags_hbm, drift_hbm, own_hbm,
    inner_ref, outer_ref, mixed_ref, power_ref, picks_ref,
    valid_ref, table_ref, lags_ref, drift_ref, own_ref, sems, rows32, masked,
):
    det_index = lax.axis_index("det")
    bin_half, detector_bit = det_index % 2, det_index // 2
    copies = fetch(
        (table_hbm, own_hbm, valid_hbm, lags_hbm, drift_hbm),
        (table_ref, own_ref, valid_ref, lags_ref, drift_ref),
        sems,
    )
    outer = width // INNER
    inner_at, start_at = inner_rows(), start_rows(outer)
    flip = jnp.where(detector_bit == 0, 1.0, -1.0).astype(jnp.float32)
    copies[0].wait()
    copies[1].wait()

    def band_of(slot):
        return table_ref[0, block_of(slot, table_ref, tm_count, bin_half)] - bin_half * bands_half

    for s in range(seg_kept):
        rows32[...] = own_ref[detector_bit * seg_kept + s].astype(jnp.float32)
        power_ref[s] = power_rows(rows32[...])
        mix_own(rows32, band_of, masked, mixed_ref, s, flip, outer, width)
    for copy in copies[2:]:
        copy.wait()
    marks = clock(valid_ref, tm_count, detector_bit, seg_kept)

    def one_slot(slot):
        row = block_of(slot, table_ref, tm_count, bin_half)
        band = table_ref[0, row]
        frequency = (band * width).astype(jnp.float32) + start_at
        share = (band.astype(jnp.float32) + 0.5) / (2 * bands_half)
        picks_ref[slot : slot + 1, :] = jnp.full((1, LANES), band_of(slot))
        for m in range(TPB):
            tile = table_ref[1, row + m]
            at = slot * TPB + m
            picks_ref[slots + at : slots + at + 1, :] = jnp.full((1, LANES), tile)
            lag, parts = inner_tables(tile, lags_ref, inner_at)
            inner_ref[at] = jnp.concatenate(parts, 0)
            for s, (live, time) in enumerate(marks):
                cosine, sine = outer_tables(tile, lag, drift_ref, share * time, frequency, live)
                outer_ref[at, s, 0] = cosine
                outer_ref[at, s, 1] = sine

    slots = inner_ref.shape[0] // TPB
    over_slots(slots, one_slot)


def terms_kernel(tm_count, dests, rows_dest, seg_kept, ready, *refs):
    if ready:
        inner_ref, outer_ref, mixed_ref, power_ref, picks_ref, other_ref, out_ref, *scratch = refs
        copies = ()
    else:
        valid_hbm, table_hbm, lags_hbm, drift_hbm, own_ref, other_ref, out_ref, *scratch = refs
        valid_ref, table_ref, lags_ref, drift_ref, sems, mixed_ref, *scratch = scratch
        copies = fetch((valid_hbm, table_hbm, lags_hbm, drift_hbm), (valid_ref, table_ref, lags_ref, drift_ref), sems)
    rows32, masked, left, total = scratch
    det_index = lax.axis_index("det")
    bin_half, detector_bit = det_index % 2, det_index // 2
    bands_half = other_ref.shape[1] // 2
    width = other_ref.shape[2]
    outer = width // INNER
    per_tile = PT // LANES
    slots = masked.shape[0]
    flip = jnp.where(detector_bit == 0, 1.0, -1.0).astype(jnp.float32)
    part = lax.broadcasted_iota(jnp.int32, (slots, outer, LANES), 2) // INNER
    total[...] = jnp.zeros_like(total)

    def band_of(slot):
        if ready:
            return picks_ref[slot : slot + 1, :][0, 0]
        return table_ref[0, block_of(slot, table_ref, tm_count, bin_half)] - bin_half * bands_half

    def tile_of(at):
        if ready:
            return picks_ref[slots + at : slots + at + 1, :][0, 0]
        return table_ref[1, block_of(at // TPB, table_ref, tm_count, bin_half) + at % TPB]

    for s in range(seg_kept):
        seg = detector_bit * seg_kept + s
        rows32[...] = other_ref[seg].astype(jnp.float32)
        powers = [power_ref[s] if ready else power_rows(own_ref[seg].astype(jnp.float32)), power_rows(rows32[...])]
        if s == 0:
            for copy in copies:
                copy.wait()
        wide = spread(rows32, band_of, masked, outer, width)
        if not ready:
            rows32[...] = own_ref[seg].astype(jnp.float32)
            mix_own(rows32, band_of, masked, mixed_ref, s, flip, outer, width)
            inner_at, start_at = inner_rows(), start_rows(outer)
            live, time = clock(valid_ref, tm_count, detector_bit, seg_kept)[s]
        real, imag = wide[:, :outer], wide[:, outer:]
        for n in range(2):
            value = mixed_ref[s, 2 * n] * real + mixed_ref[s, 2 * n + 1] * imag
            high = value.astype(jnp.bfloat16).astype(jnp.float32)
            parts = jnp.where((part == 2) | (part == 3), value - high, high)
            left[:, n * outer : (n + 1) * outer, :] = parts

        def one_slot(slot):
            lhs = left[slot][:, : PARTS * INNER].astype(jnp.bfloat16)
            for m in range(TPB):
                at = slot * TPB + m
                tile = tile_of(at)
                if ready:
                    table = inner_ref[at]
                    cosine, sine = outer_ref[at, s, 0], outer_ref[at, s, 1]
                else:
                    band = band_of(slot) + bin_half * bands_half
                    lag, parts = inner_tables(tile, lags_ref, inner_at)
                    table = jnp.concatenate(parts, 0)
                    turn = (band.astype(jnp.float32) + 0.5) / (2 * bands_half) * time
                    frequency = (band * width).astype(jnp.float32) + start_at
                    cosine, sine = outer_tables(tile, lag, drift_ref, turn, frequency, live)
                rhs = jnp.concatenate([table[: 2 * INNER], table], 0)
                product = jnp.dot(lhs, rhs, preferred_element_type=jnp.float32)
                terms = jnp.sum(cosine * product[:outer] - sine * product[outer:], axis=0, keepdims=True)
                total[s, tile] += jnp.concatenate([terms[:, c * LANES : (c + 1) * LANES] for c in range(per_tile)], 0)

        over_slots(slots, one_slot)
        tiles = rows_dest // per_tile
        powers = jnp.concatenate(powers, 0)
        for d in range(dests):
            piece = total[s, d * tiles : (d + 1) * tiles].reshape(rows_dest, LANES)
            out_ref[d, s] = jnp.concatenate([piece, powers], 0).astype(jnp.bfloat16)


def weights_of(power, fourier_bins):
    halves = power[..., 0::2, :] + power[..., 1::2, :]
    whole = halves.reshape(2, 2, *halves.shape[1:]).sum(1) / fourier_bins + 1e-06
    return 1.0 / (whole[..., 0, :] * whole[..., 1, :])


def sum_kernel(tm_count, rows_dest, fourier_bins, scale, got_ref, out_ref):
    seg_kept = got_ref.shape[1]
    total = jnp.zeros((rows_dest, LANES), jnp.float32)
    for k in range(2):
        for i in range(tm_count):
            for s in range(seg_kept):
                pair = [got_ref[(2 * k + h) * tm_count + i, s].astype(jnp.float32) for h in range(2)]
                both = pair[0] + pair[1]
                own = (both[rows_dest : rows_dest + 1] + both[rows_dest + 1 : rows_dest + 2]) / fourier_bins + 1e-06
                other = (both[rows_dest + 2 : rows_dest + 3] + both[rows_dest + 3 : rows_dest + 4]) / fourier_bins + 1e-06
                total = total + both[:rows_dest] * (1.0 / (own * other))
    out_ref[...] = total / scale


def shards(spectra, valid, lags, drift, block_table):
    det_count, tm_count = lax.axis_size("det"), lax.axis_size("tm")
    devices = det_count * tm_count
    own = spectra[0]
    seg_count, bands_half, _, width = own.shape
    seg_kept = seg_count // 2
    pixels = lags.shape[0]
    per_device = pixels // devices
    fourier_bins = 2 * bands_half * width
    scale = math.sqrt(seg_count * tm_count * width)
    direct = per_device % PT == 0
    rows_dest = (per_device if direct else pixels) // LANES
    dests = devices if direct else 1
    rows = rows_dest + 4
    per_tile = PT // LANES
    blocks = block_table.shape[0] // 2
    slots = blocks // TPB
    outer = width // INNER

    own = own.reshape(seg_count, 2 * bands_half, width)
    other = lax.ppermute(own, "det", [(d, d ^ 2) for d in range(det_count)])
    table = block_table.T
    lags, drift = (x.reshape(-1, per_tile, LANES) for x in (lags, drift))
    settings = tuple(pltpu.with_memory_space_constraint(x, pltpu.HBM) for x in (valid, table, lags, drift))
    held = [pltpu.SMEM(valid.shape, jnp.int32), pltpu.SMEM(table.shape, jnp.int32)]
    held += [pltpu.VMEM(lags.shape, jnp.float32), pltpu.VMEM(drift.shape, jnp.float32)]
    work = [pltpu.VMEM(own.shape[1:], jnp.float32), pltpu.VMEM((slots, 2 * outer, width), jnp.bfloat16)]
    mixed = jax.ShapeDtypeStruct((seg_kept, 4, slots, outer, LANES), jnp.float32)
    ready = slots <= UNROLLED
    if ready:
        made = pl.pallas_call(
            functools.partial(tables_kernel, tm_count, bands_half, width, seg_kept),
            out_shape=[
                jax.ShapeDtypeStruct((blocks, 4 * INNER, PT), jnp.bfloat16),
                jax.ShapeDtypeStruct((blocks, seg_kept, 2, outer, PT), jnp.float32),
                mixed,
                jax.ShapeDtypeStruct((seg_kept, 2, LANES), jnp.float32),
                jax.ShapeDtypeStruct((slots + blocks, LANES), jnp.int32),
            ],
            in_specs=[HBM] * 5,
            out_specs=[VMEM] * 5,
            scratch_shapes=[*held, pltpu.VMEM(own.shape, own.dtype), pltpu.SemaphoreType.DMA((5,)), *work],
            compiler_params=GRANT,
            cost_estimate=pl.CostEstimate(flops=10**9, bytes_accessed=10**6, transcendentals=0),
            name="tables",
        )(*settings, pltpu.with_memory_space_constraint(own, pltpu.HBM))
        settings, held = made, []
    else:
        settings = (*settings, own)
        held += [pltpu.SemaphoreType.DMA((4,)), pltpu.VMEM(mixed.shape, mixed.dtype)]
    outgoing = pl.pallas_call(
        functools.partial(terms_kernel, tm_count, dests, rows_dest, seg_kept, ready),
        out_shape=jax.ShapeDtypeStruct((dests, seg_kept, rows, LANES), jnp.bfloat16),
        in_specs=([VMEM] * 5 if ready else [HBM] * 4 + [VMEM]) + [VMEM],
        out_specs=VMEM,
        scratch_shapes=[
            *held,
            *work,
            pltpu.VMEM((slots, 2 * outer, LANES), jnp.float32),
            pltpu.VMEM((seg_kept, pixels // PT, per_tile, LANES), jnp.float32),
        ],
        compiler_params=GRANT if ready else None,
        name="terms",
    )(*settings, other)
    if direct:
        received = lax.all_to_all(outgoing, ("det", "tm"), 0, 0, tiled=True)
        result = pl.pallas_call(
            functools.partial(sum_kernel, tm_count, rows_dest, fourier_bins, scale),
            out_shape=jax.ShapeDtypeStruct((rows_dest, LANES), jnp.float32),
            in_specs=[VMEM],
            out_specs=VMEM,
            compiler_params=GRANT,
            name="sum",
        )(received)
        return result.reshape(-1)
    maps = jnp.moveaxis(outgoing[0, :, :rows_dest].reshape(seg_kept, devices, per_device), 1, 0)
    powers = jnp.broadcast_to(outgoing[0, :, rows_dest : rows_dest + 4, 0], (devices, seg_kept, 4))
    sent = jnp.concatenate([maps, powers], 2)
    received = lax.all_to_all(sent, ("det", "tm"), 0, 0, tiled=True).astype(jnp.float32)
    received = received.reshape(det_count, tm_count, seg_kept, per_device + 4)
    weight = weights_of(received[..., per_device:, None], fourier_bins)[..., 0]
    both = received[..., :per_device].reshape(2, 2, tm_count, seg_kept, per_device).sum(1)
    return (both * weight[..., None]).sum((0, 1, 2)) / scale


def solution(mesh):
    placed = (P("det", "tm", None, None, None), P("tm"), P(), P(), P())
    return jax.shard_map(
        shards, mesh=mesh, in_specs=placed, out_specs=P(("det", "tm")), check_vma=False
    )
```

```python
import functools
import math

import jax
import jax.numpy as jnp
import numpy as np
from jax import lax
from jax.experimental import pallas as pl
from jax.experimental.pallas import tpu as pltpu
from jax.sharding import PartitionSpec as P

PT = 512
TPB = 2
LANES = 128
INNER = 16
HALF = INNER // 2
PARTS = 6
UNROLLED = 16
GRANT = pltpu.CompilerParams(vmem_limit_bytes=8 << 20)

VMEM = pl.BlockSpec(memory_space=pltpu.VMEM)
HBM = pl.BlockSpec(memory_space=pltpu.HBM)


def fitted(function, limit, degree):
    nodes = (np.cos(np.pi * (np.arange(400) + 0.5) / 400) + 1) / 2
    powers = np.vander(nodes, degree + 1, increasing=True)
    coefficients = np.linalg.lstsq(powers, function(np.sqrt(nodes * limit)), rcond=None)[0]
    return tuple(float(c) for c in coefficients / limit ** np.arange(degree + 1))


NEAR_COS = fitted(lambda r: np.cos(2 * np.pi * r), 0.0064, 3)
NEAR_SIN = fitted(lambda r: np.sin(2 * np.pi * r) / r, 0.0064, 3)
FAR_COS = fitted(lambda r: np.cos(2 * np.pi * r), 0.25, 6)
FAR_SIN = fitted(lambda r: np.sin(2 * np.pi * r) / r, 0.25, 6)


def horner(coefficients, z):
    total = jnp.full_like(z, coefficients[-1])
    for c in coefficients[-2::-1]:
        total = total * z + c
    return total


def near_turn(x):
    z = x * x
    return horner(NEAR_COS, z), x * horner(NEAR_SIN, z)


def any_turn(x):
    r = x - jnp.floor(x + 0.5)
    z = r * r
    return horner(FAR_COS, z), r * horner(FAR_SIN, z)


def split(x):
    high = x.astype(jnp.bfloat16)
    return high, (x - high.astype(jnp.float32)).astype(jnp.bfloat16)


def block_of(slot, table_ref, tm_count, bin_half):
    per_group = table_ref.shape[1] // (2 * tm_count)
    first = slot * TPB
    return (2 * (first // per_group) + bin_half) * per_group + first % per_group


def over_slots(slots, one_slot):
    if slots <= UNROLLED:
        for slot in range(slots):
            one_slot(slot)
    else:
        lax.fori_loop(0, slots, lambda slot, _: (one_slot(slot), 0)[1], 0)


def inner_tables(tile, lags_ref, inner_at):
    lag = jnp.concatenate([lags_ref[tile, c : c + 1, :] for c in range(PT // LANES)], 1)
    cosine, sine = near_turn(jnp.broadcast_to(lag, inner_at.shape) * inner_at)
    return lag, jnp.concatenate(split(jnp.concatenate([cosine, sine], 0)), 0)


def outer_tables(tile, lag, drift_ref, turn, frequency, live):
    pace = jnp.concatenate([drift_ref[tile, c : c + 1, :] for c in range(PT // LANES)], 1)
    shape = frequency.shape
    cosine, sine = any_turn(jnp.broadcast_to(pace * turn, shape) - frequency * jnp.broadcast_to(lag, shape))
    return cosine * live, sine * live


def clock(valid_ref, tm_count, detector_bit, seg_kept):
    tm_index = lax.axis_index("tm")
    seg_count = valid_ref.shape[0]
    segment_total = seg_count * tm_count
    marks = []
    for s in range(seg_kept):
        seg = detector_bit * seg_kept + s
        time = ((tm_index * seg_count + seg).astype(jnp.float32) + 0.5 - segment_total / 2) / segment_total
        marks.append((valid_ref[seg].astype(jnp.float32), time))
    return marks


def fetch(sources, targets, sems):
    copies = [pltpu.make_async_copy(a, b, sems.at[n]) for n, (a, b) in enumerate(zip(sources, targets))]
    for copy in copies:
        copy.start()
    return copies


def start_rows(outer):
    return (lax.broadcasted_iota(jnp.int32, (outer, PT), 0) * INNER).astype(jnp.float32) + (INNER - 1) / 2


def inner_rows():
    return lax.broadcasted_iota(jnp.int32, (HALF, PT), 0).astype(jnp.float32) + 0.5


def spread(rows_ref, band_of, masked, outer, width):
    lane_at = lax.broadcasted_iota(jnp.int32, (outer, width), 1)
    mask = (lane_at // INNER == lax.broadcasted_iota(jnp.int32, (outer, width), 0)).astype(jnp.float32)
    from_lane = lax.broadcasted_iota(jnp.int32, (width, LANES), 0) % INNER
    to_lane = lax.broadcasted_iota(jnp.int32, (width, LANES), 1) % HALF
    choose = jnp.concatenate([from_lane == HALF + to_lane, from_lane == HALF - 1 - to_lane], 1)

    def one_slot(slot):
        row = 2 * band_of(slot)
        pair = [jnp.broadcast_to(rows_ref[pl.ds(row + c, 1), :], (outer, width)) * mask for c in range(2)]
        return jnp.concatenate(pair, 0).astype(jnp.bfloat16)

    slots = masked.shape[0]
    if slots <= UNROLLED:
        stacked = jnp.concatenate([one_slot(slot) for slot in range(slots)], 0)
    else:
        def kept(slot):
            masked[slot] = one_slot(slot)

        over_slots(slots, kept)
        stacked = masked[...].reshape(slots * 2 * outer, width)
    wide = jnp.dot(stacked, choose.astype(jnp.float32).astype(jnp.bfloat16), preferred_element_type=jnp.float32)
    wide = wide.reshape(slots, 2 * outer, 2 * LANES)
    return [wide[:, c * outer : (c + 1) * outer, m * LANES : (m + 1) * LANES] for m in range(2) for c in range(2)]


def mix_own(rows_ref, band_of, masked, mixed_ref, s, flip, outer, width):
    real, imag, real_m, imag_m = spread(rows_ref, band_of, masked, outer, width)
    even = lax.broadcasted_iota(jnp.int32, real.shape, 2) // HALF % 2 == 0
    turned, turned_m = flip * imag, flip * imag_m
    kept, kept_m = flip * real, flip * real_m
    factors = (
        (real, -turned), (imag, kept), (real_m, turned_m), (imag_m, -kept_m),
        (-turned, -real), (kept, -imag), (-turned_m, real_m), (kept_m, imag_m),
    )
    for n, (first, second) in enumerate(factors):
        mixed_ref[s, n] = jnp.where(even, first, second)


def power_rows(rows):
    power = jnp.sum(jnp.sum(rows * rows, axis=0, keepdims=True), axis=1, keepdims=True)
    high = power.astype(jnp.bfloat16).astype(jnp.float32)
    return jnp.concatenate([jnp.broadcast_to(x, (1, LANES)) for x in (high, power - high)], 0)


def tables_kernel(
    tm_count, bands_half, width, seg_kept,
    valid_hbm, table_hbm, lags_hbm, drift_hbm, own_hbm,
    inner_ref, outer_ref, mixed_ref, power_ref, picks_ref,
    valid_ref, table_ref, lags_ref, drift_ref, own_ref, sems, rows32, masked,
):
    det_index = lax.axis_index("det")
    bin_half, detector_bit = det_index % 2, det_index // 2
    copies = fetch(
        (table_hbm, own_hbm, valid_hbm, lags_hbm, drift_hbm),
        (table_ref, own_ref, valid_ref, lags_ref, drift_ref),
        sems,
    )
    outer = width // INNER
    inner_at, start_at = inner_rows(), start_rows(outer)
    flip = jnp.where(detector_bit == 0, 1.0, -1.0).astype(jnp.float32)
    copies[0].wait()
    copies[1].wait()

    def band_of(slot):
        return table_ref[0, block_of(slot, table_ref, tm_count, bin_half)] - bin_half * bands_half

    for s in range(seg_kept):
        rows32[...] = own_ref[detector_bit * seg_kept + s].astype(jnp.float32)
        power_ref[s] = power_rows(rows32[...])
        mix_own(rows32, band_of, masked, mixed_ref, s, flip, outer, width)
    for copy in copies[2:]:
        copy.wait()
    marks = clock(valid_ref, tm_count, detector_bit, seg_kept)

    def one_slot(slot):
        row = block_of(slot, table_ref, tm_count, bin_half)
        band = table_ref[0, row]
        frequency = (band * width).astype(jnp.float32) + start_at
        share = (band.astype(jnp.float32) + 0.5) / (2 * bands_half)
        picks_ref[slot : slot + 1, :] = jnp.full((1, LANES), band_of(slot))
        for m in range(TPB):
            tile = table_ref[1, row + m]
            at = slot * TPB + m
            picks_ref[slots + at : slots + at + 1, :] = jnp.full((1, LANES), tile)
            lag, parts = inner_tables(tile, lags_ref, inner_at)
            inner_ref[at] = parts
            for s, (live, time) in enumerate(marks):
                cosine, sine = outer_tables(tile, lag, drift_ref, share * time, frequency, live)
                outer_ref[at, s, 0] = cosine
                outer_ref[at, s, 1] = sine

    slots = inner_ref.shape[0] // TPB
    over_slots(slots, one_slot)


def terms_kernel(tm_count, dests, rows_dest, seg_kept, ready, *refs):
    if ready:
        inner_ref, outer_ref, mixed_ref, power_ref, picks_ref, other_ref, out_ref, *scratch = refs
        copies = ()
    else:
        valid_hbm, table_hbm, lags_hbm, drift_hbm, own_ref, other_ref, out_ref, *scratch = refs
        valid_ref, table_ref, lags_ref, drift_ref, sems, mixed_ref, *scratch = scratch
        copies = fetch((valid_hbm, table_hbm, lags_hbm, drift_hbm), (valid_ref, table_ref, lags_ref, drift_ref), sems)
    rows32, masked, left, total = scratch
    det_index = lax.axis_index("det")
    bin_half, detector_bit = det_index % 2, det_index // 2
    bands_half = other_ref.shape[1] // 2
    width = other_ref.shape[2]
    outer = width // INNER
    per_tile = PT // LANES
    slots = masked.shape[0]
    flip = jnp.where(detector_bit == 0, 1.0, -1.0).astype(jnp.float32)
    part = lax.broadcasted_iota(jnp.int32, (slots, outer, LANES), 2) // HALF
    total[...] = jnp.zeros_like(total)

    def band_of(slot):
        if ready:
            return picks_ref[slot : slot + 1, :][0, 0]
        return table_ref[0, block_of(slot, table_ref, tm_count, bin_half)] - bin_half * bands_half

    def tile_of(at):
        if ready:
            return picks_ref[slots + at : slots + at + 1, :][0, 0]
        return table_ref[1, block_of(at // TPB, table_ref, tm_count, bin_half) + at % TPB]

    for s in range(seg_kept):
        seg = detector_bit * seg_kept + s
        rows32[...] = other_ref[seg].astype(jnp.float32)
        powers = [power_ref[s] if ready else power_rows(own_ref[seg].astype(jnp.float32)), power_rows(rows32[...])]
        if s == 0:
            for copy in copies:
                copy.wait()
        wide = spread(rows32, band_of, masked, outer, width)
        if not ready:
            rows32[...] = own_ref[seg].astype(jnp.float32)
            mix_own(rows32, band_of, masked, mixed_ref, s, flip, outer, width)
            inner_at, start_at = inner_rows(), start_rows(outer)
            live, time = clock(valid_ref, tm_count, detector_bit, seg_kept)[s]
        sides = []
        for n in range(2):
            value = sum(mixed_ref[s, 4 * n + q] * wide[q] for q in range(4))
            high = value.astype(jnp.bfloat16).astype(jnp.float32)
            sides.append(jnp.where((part == 2) | (part == 3), value - high, high))
        left[...] = jnp.concatenate(sides, 1).astype(jnp.bfloat16)

        def one_slot(slot):
            lhs = left[slot][:, : PARTS * HALF]
            for m in range(TPB):
                at = slot * TPB + m
                tile = tile_of(at)
                if ready:
                    table = inner_ref[at]
                    cosine, sine = outer_ref[at, s, 0], outer_ref[at, s, 1]
                else:
                    band = band_of(slot) + bin_half * bands_half
                    lag, table = inner_tables(tile, lags_ref, inner_at)
                    turn = (band.astype(jnp.float32) + 0.5) / (2 * bands_half) * time
                    frequency = (band * width).astype(jnp.float32) + start_at
                    cosine, sine = outer_tables(tile, lag, drift_ref, turn, frequency, live)
                rhs = jnp.concatenate([table[:INNER], table], 0)
                product = jnp.dot(lhs, rhs, preferred_element_type=jnp.float32)
                terms = jnp.sum(cosine * product[:outer] - sine * product[outer:], axis=0, keepdims=True)
                total[s, tile] += jnp.concatenate([terms[:, c * LANES : (c + 1) * LANES] for c in range(per_tile)], 0)

        over_slots(slots, one_slot)
        tiles = rows_dest // per_tile
        powers = jnp.concatenate(powers, 0)
        for d in range(dests):
            piece = total[s, d * tiles : (d + 1) * tiles].reshape(rows_dest, LANES)
            out_ref[d, s] = jnp.concatenate([piece, powers], 0).astype(jnp.bfloat16)


def weights_of(power, fourier_bins):
    halves = power[..., 0::2, :] + power[..., 1::2, :]
    whole = halves.reshape(2, 2, *halves.shape[1:]).sum(1) / fourier_bins + 1e-06
    return 1.0 / (whole[..., 0, :] * whole[..., 1, :])


def sum_kernel(tm_count, rows_dest, fourier_bins, scale, got_ref, out_ref):
    seg_kept = got_ref.shape[1]
    total = jnp.zeros((rows_dest, LANES), jnp.float32)
    for k in range(2):
        for i in range(tm_count):
            for s in range(seg_kept):
                pair = [got_ref[(2 * k + h) * tm_count + i, s].astype(jnp.float32) for h in range(2)]
                both = pair[0] + pair[1]
                own = (both[rows_dest : rows_dest + 1] + both[rows_dest + 1 : rows_dest + 2]) / fourier_bins + 1e-06
                other = (both[rows_dest + 2 : rows_dest + 3] + both[rows_dest + 3 : rows_dest + 4]) / fourier_bins + 1e-06
                total = total + both[:rows_dest] * (1.0 / (own * other))
    out_ref[...] = total / scale


def shards(spectra, valid, lags, drift, block_table):
    det_count, tm_count = lax.axis_size("det"), lax.axis_size("tm")
    devices = det_count * tm_count
    own = spectra[0]
    seg_count, bands_half, _, width = own.shape
    seg_kept = seg_count // 2
    pixels = lags.shape[0]
    per_device = pixels // devices
    fourier_bins = 2 * bands_half * width
    scale = math.sqrt(seg_count * tm_count * width)
    direct = per_device % PT == 0
    rows_dest = (per_device if direct else pixels) // LANES
    dests = devices if direct else 1
    rows = rows_dest + 4
    per_tile = PT // LANES
    blocks = block_table.shape[0] // 2
    slots = blocks // TPB
    outer = width // INNER

    own = own.reshape(seg_count, 2 * bands_half, width)
    other = lax.ppermute(own, "det", [(d, d ^ 2) for d in range(det_count)])
    table = block_table.T
    lags, drift = (x.reshape(-1, per_tile, LANES) for x in (lags, drift))
    settings = tuple(pltpu.with_memory_space_constraint(x, pltpu.HBM) for x in (valid, table, lags, drift))
    held = [pltpu.SMEM(valid.shape, jnp.int32), pltpu.SMEM(table.shape, jnp.int32)]
    held += [pltpu.VMEM(lags.shape, jnp.float32), pltpu.VMEM(drift.shape, jnp.float32)]
    work = [pltpu.VMEM(own.shape[1:], jnp.float32), pltpu.VMEM((slots, 2 * outer, width), jnp.bfloat16)]
    mixed = jax.ShapeDtypeStruct((seg_kept, 8, slots, outer, LANES), jnp.float32)
    ready = slots <= UNROLLED
    if ready:
        made = pl.pallas_call(
            functools.partial(tables_kernel, tm_count, bands_half, width, seg_kept),
            out_shape=[
                jax.ShapeDtypeStruct((blocks, 2 * INNER, PT), jnp.bfloat16),
                jax.ShapeDtypeStruct((blocks, seg_kept, 2, outer, PT), jnp.float32),
                mixed,
                jax.ShapeDtypeStruct((seg_kept, 2, LANES), jnp.float32),
                jax.ShapeDtypeStruct((slots + blocks, LANES), jnp.int32),
            ],
            in_specs=[HBM] * 5,
            out_specs=[VMEM] * 5,
            scratch_shapes=[*held, pltpu.VMEM(own.shape, own.dtype), pltpu.SemaphoreType.DMA((5,)), *work],
            compiler_params=GRANT,
            cost_estimate=pl.CostEstimate(flops=10**9, bytes_accessed=10**6, transcendentals=0),
            name="tables",
        )(*settings, pltpu.with_memory_space_constraint(own, pltpu.HBM))
        settings, held = made, []
    else:
        settings = (*settings, own)
        held += [pltpu.SemaphoreType.DMA((4,)), pltpu.VMEM(mixed.shape, mixed.dtype)]
    outgoing = pl.pallas_call(
        functools.partial(terms_kernel, tm_count, dests, rows_dest, seg_kept, ready),
        out_shape=jax.ShapeDtypeStruct((dests, seg_kept, rows, LANES), jnp.bfloat16),
        in_specs=([VMEM] * 5 if ready else [HBM] * 4 + [VMEM]) + [VMEM],
        out_specs=VMEM,
        scratch_shapes=[
            *held,
            *work,
            pltpu.VMEM((slots, 2 * outer, LANES), jnp.bfloat16),
            pltpu.VMEM((seg_kept, pixels // PT, per_tile, LANES), jnp.float32),
        ],
        compiler_params=GRANT if ready else None,
        name="terms",
    )(*settings, other)
    if direct:
        received = lax.all_to_all(outgoing, ("det", "tm"), 0, 0, tiled=True)
        result = pl.pallas_call(
            functools.partial(sum_kernel, tm_count, rows_dest, fourier_bins, scale),
            out_shape=jax.ShapeDtypeStruct((rows_dest, LANES), jnp.float32),
            in_specs=[VMEM],
            out_specs=VMEM,
            compiler_params=GRANT,
            name="sum",
        )(received)
        return result.reshape(-1)
    maps = jnp.moveaxis(outgoing[0, :, :rows_dest].reshape(seg_kept, devices, per_device), 1, 0)
    powers = jnp.broadcast_to(outgoing[0, :, rows_dest : rows_dest + 4, 0], (devices, seg_kept, 4))
    sent = jnp.concatenate([maps, powers], 2)
    received = lax.all_to_all(sent, ("det", "tm"), 0, 0, tiled=True).astype(jnp.float32)
    received = received.reshape(det_count, tm_count, seg_kept, per_device + 4)
    weight = weights_of(received[..., per_device:, None], fourier_bins)[..., 0]
    both = received[..., :per_device].reshape(2, 2, tm_count, seg_kept, per_device).sum(1)
    return (both * weight[..., None]).sum((0, 1, 2)) / scale


def solution(mesh):
    placed = (P("det", "tm", None, None, None), P("tm"), P(), P(), P())
    return jax.shard_map(
        shards, mesh=mesh, in_specs=placed, out_specs=P(("det", "tm")), check_vma=False
    )
```

```python
import functools
import math

import jax
import jax.numpy as jnp
import numpy as np
from jax import lax
from jax.experimental import pallas as pl
from jax.experimental.pallas import tpu as pltpu
from jax.sharding import PartitionSpec as P


PT = 512
TPB = 2
LANES = 128
INNER = 16
HALF = INNER // 2
PARTS = 6
UNROLLED = 16
GRANT = pltpu.CompilerParams(vmem_limit_bytes=8 << 20)

VMEM = pl.BlockSpec(memory_space=pltpu.VMEM)
HBM = pl.BlockSpec(memory_space=pltpu.HBM)


def fitted(function, limit, degree):
    nodes = (np.cos(np.pi * (np.arange(400) + 0.5) / 400) + 1) / 2
    powers = np.vander(nodes, degree + 1, increasing=True)
    coefficients = np.linalg.lstsq(powers, function(np.sqrt(nodes * limit)), rcond=None)[0]
    return tuple(float(c) for c in coefficients / limit ** np.arange(degree + 1))


NEAR_COS = fitted(lambda r: np.cos(2 * np.pi * r), 0.0064, 3)
NEAR_SIN = fitted(lambda r: np.sin(2 * np.pi * r) / r, 0.0064, 3)
FAR_COS = fitted(lambda r: np.cos(2 * np.pi * r), 0.25, 6)
FAR_SIN = fitted(lambda r: np.sin(2 * np.pi * r) / r, 0.25, 6)


def horner(coefficients, z):
    total = jnp.full_like(z, coefficients[-1])
    for c in coefficients[-2::-1]:
        total = total * z + c
    return total


def near_turn(x):
    z = x * x
    return horner(NEAR_COS, z), x * horner(NEAR_SIN, z)


def any_turn(x):
    r = x - jnp.floor(x + 0.5)
    z = r * r
    return horner(FAR_COS, z), r * horner(FAR_SIN, z)


def split(x):
    high = x.astype(jnp.bfloat16)
    return high, (x - high.astype(jnp.float32)).astype(jnp.bfloat16)


def block_of(slot, table_ref, tm_count, bin_half):
    per_group = table_ref.shape[1] // (2 * tm_count)
    first = slot * TPB
    return (2 * (first // per_group) + bin_half) * per_group + first % per_group


def over_slots(slots, one_slot):
    if slots <= UNROLLED:
        for slot in range(slots):
            one_slot(slot)
    else:
        lax.fori_loop(0, slots, lambda slot, _: (one_slot(slot), 0)[1], 0)


def inner_tables(tile, lags_ref, inner_at):
    lag = jnp.concatenate([lags_ref[tile, c : c + 1, :] for c in range(PT // LANES)], 1)
    cosine, sine = near_turn(jnp.broadcast_to(lag, inner_at.shape) * inner_at)
    return lag, jnp.concatenate(split(jnp.concatenate([cosine, sine], 0)), 0)


def outer_tables(tile, lag, drift_ref, turn, frequency, live):
    pace = jnp.concatenate([drift_ref[tile, c : c + 1, :] for c in range(PT // LANES)], 1)
    shape = frequency.shape
    cosine, sine = any_turn(jnp.broadcast_to(pace * turn, shape) - frequency * jnp.broadcast_to(lag, shape))
    return cosine * live, sine * live


def duty():
    det_index = lax.axis_index("det")
    return 1 - det_index % 2, det_index // 2


def clock(valid_ref, tm_count, detector_bit, seg_kept):
    tm_index = lax.axis_index("tm")
    seg_count = valid_ref.shape[0]
    segment_total = seg_count * tm_count
    marks = []
    for s in range(seg_kept):
        seg = detector_bit * seg_kept + s
        time = ((tm_index * seg_count + seg).astype(jnp.float32) + 0.5 - segment_total / 2) / segment_total
        marks.append((valid_ref[seg].astype(jnp.float32), time))
    return marks


def fetch(sources, targets, sems):
    copies = [pltpu.make_async_copy(a, b, sems.at[n]) for n, (a, b) in enumerate(zip(sources, targets))]
    for copy in copies:
        copy.start()
    return copies


def start_rows(outer):
    return (lax.broadcasted_iota(jnp.int32, (outer, PT), 0) * INNER).astype(jnp.float32) + (INNER - 1) / 2


def inner_rows():
    return lax.broadcasted_iota(jnp.int32, (HALF, PT), 0).astype(jnp.float32) + 0.5


def spread(rows_ref, band_of, masked, outer, width):
    lane_at = lax.broadcasted_iota(jnp.int32, (outer, width), 1)
    mask = (lane_at // INNER == lax.broadcasted_iota(jnp.int32, (outer, width), 0)).astype(jnp.float32)
    from_lane = lax.broadcasted_iota(jnp.int32, (width, LANES), 0) % INNER
    to_lane = lax.broadcasted_iota(jnp.int32, (width, LANES), 1) % HALF
    choose = jnp.concatenate([from_lane == HALF + to_lane, from_lane == HALF - 1 - to_lane], 1)

    def one_slot(slot):
        row = 2 * band_of(slot)
        pair = [jnp.broadcast_to(rows_ref[pl.ds(row + c, 1), :], (outer, width)) * mask for c in range(2)]
        return jnp.concatenate(pair, 0).astype(jnp.bfloat16)

    slots = masked.shape[0]
    if slots <= UNROLLED:
        stacked = jnp.concatenate([one_slot(slot) for slot in range(slots)], 0)
    else:
        def kept(slot):
            masked[slot] = one_slot(slot)

        over_slots(slots, kept)
        stacked = masked[...].reshape(slots * 2 * outer, width)
    wide = jnp.dot(stacked, choose.astype(jnp.float32).astype(jnp.bfloat16), preferred_element_type=jnp.float32)
    wide = wide.reshape(slots, 2 * outer, 2 * LANES)
    return [wide[:, c * outer : (c + 1) * outer, m * LANES : (m + 1) * LANES] for m in range(2) for c in range(2)]


def mix_own(rows_ref, band_of, masked, mixed_ref, s, flip, outer, width):
    real, imag, real_m, imag_m = spread(rows_ref, band_of, masked, outer, width)
    even = lax.broadcasted_iota(jnp.int32, real.shape, 2) // HALF % 2 == 0
    turned, turned_m = flip * imag, flip * imag_m
    kept, kept_m = flip * real, flip * real_m
    factors = (
        (real, -turned), (imag, kept), (real_m, turned_m), (imag_m, -kept_m),
        (-turned, -real), (kept, -imag), (-turned_m, real_m), (kept_m, imag_m),
    )
    for n, (first, second) in enumerate(factors):
        mixed_ref[s, n] = jnp.where(even, first, second)


def power_rows(rows):
    power = jnp.sum(jnp.sum(rows * rows, axis=0, keepdims=True), axis=1, keepdims=True)
    high = power.astype(jnp.bfloat16).astype(jnp.float32)
    return jnp.concatenate([jnp.broadcast_to(x, (1, LANES)) for x in (high, power - high)], 0)


def tables_kernel(
    tm_count, bands_half, width, seg_kept,
    valid_hbm, table_hbm, lags_hbm, drift_hbm,
    inner_ref, outer_ref, picks_ref,
    valid_ref, table_ref, lags_ref, drift_ref, sems,
):
    bin_half, detector_bit = duty()
    copies = fetch((valid_hbm, table_hbm, lags_hbm, drift_hbm), (valid_ref, table_ref, lags_ref, drift_ref), sems)
    inner_at, start_at = inner_rows(), start_rows(width // INNER)
    for copy in copies:
        copy.wait()
    marks = clock(valid_ref, tm_count, detector_bit, seg_kept)

    def one_slot(slot):
        row = block_of(slot, table_ref, tm_count, bin_half)
        band = table_ref[0, row]
        frequency = (band * width).astype(jnp.float32) + start_at
        share = (band.astype(jnp.float32) + 0.5) / (2 * bands_half)
        picks_ref[slot : slot + 1, :] = jnp.full((1, LANES), band - bin_half * bands_half)
        for m in range(TPB):
            tile = table_ref[1, row + m]
            at = slot * TPB + m
            picks_ref[slots + at : slots + at + 1, :] = jnp.full((1, LANES), tile)
            lag, parts = inner_tables(tile, lags_ref, inner_at)
            inner_ref[at] = parts
            for s, (live, time) in enumerate(marks):
                cosine, sine = outer_tables(tile, lag, drift_ref, share * time, frequency, live)
                outer_ref[at, s, 0] = cosine
                outer_ref[at, s, 1] = sine

    slots = inner_ref.shape[0] // TPB
    over_slots(slots, one_slot)


def mix_kernel(seg_kept, picks_ref, own_ref, mixed_ref, power_ref, rows32, masked):
    _, detector_bit = duty()
    _, outer = mixed_ref.shape[2:4]
    flip = jnp.where(detector_bit == 0, 1.0, -1.0).astype(jnp.float32)

    def band_of(slot):
        return picks_ref[slot : slot + 1, :][0, 0]

    for s in range(seg_kept):
        rows32[...] = own_ref[detector_bit * seg_kept + s].astype(jnp.float32)
        power_ref[s] = power_rows(rows32[...])
        mix_own(rows32, band_of, masked, mixed_ref, s, flip, outer, own_ref.shape[2])


def terms_kernel(tm_count, dests, rows_dest, seg_kept, ready, *refs):
    if ready:
        inner_ref, outer_ref, picks_ref, mixed_ref, power_ref, other_ref, out_ref, *scratch = refs
        copies = ()
    else:
        valid_hbm, table_hbm, lags_hbm, drift_hbm, own_ref, other_ref, out_ref, *scratch = refs
        valid_ref, table_ref, lags_ref, drift_ref, sems, mixed_ref, *scratch = scratch
        copies = fetch((valid_hbm, table_hbm, lags_hbm, drift_hbm), (valid_ref, table_ref, lags_ref, drift_ref), sems)
    rows32, masked, left, total = scratch
    bin_half, detector_bit = duty()
    bands_half = other_ref.shape[1] // 2
    width = other_ref.shape[2]
    outer = width // INNER
    per_tile = PT // LANES
    slots = masked.shape[0]
    flip = jnp.where(detector_bit == 0, 1.0, -1.0).astype(jnp.float32)
    part = lax.broadcasted_iota(jnp.int32, (slots, outer, LANES), 2) // HALF
    total[...] = jnp.zeros_like(total)

    def band_of(slot):
        if ready:
            return picks_ref[slot : slot + 1, :][0, 0]
        return table_ref[0, block_of(slot, table_ref, tm_count, bin_half)] - bin_half * bands_half

    def tile_of(at):
        if ready:
            return picks_ref[slots + at : slots + at + 1, :][0, 0]
        return table_ref[1, block_of(at // TPB, table_ref, tm_count, bin_half) + at % TPB]

    for s in range(seg_kept):
        seg = detector_bit * seg_kept + s
        rows32[...] = other_ref[seg].astype(jnp.float32)
        powers = [power_ref[s] if ready else power_rows(own_ref[seg].astype(jnp.float32)), power_rows(rows32[...])]
        if s == 0:
            for copy in copies:
                copy.wait()
        wide = spread(rows32, band_of, masked, outer, width)
        if not ready:
            rows32[...] = own_ref[seg].astype(jnp.float32)
            mix_own(rows32, band_of, masked, mixed_ref, s, flip, outer, width)
            inner_at, start_at = inner_rows(), start_rows(outer)
            live, time = clock(valid_ref, tm_count, detector_bit, seg_kept)[s]
        sides = []
        for n in range(2):
            value = sum(mixed_ref[s, 4 * n + q] * wide[q] for q in range(4))
            high = value.astype(jnp.bfloat16).astype(jnp.float32)
            sides.append(jnp.where((part == 2) | (part == 3), value - high, high))
        left[...] = jnp.concatenate(sides, 1).astype(jnp.bfloat16)

        def one_slot(slot):
            lhs = left[slot][:, : PARTS * HALF]
            for m in range(TPB):
                at = slot * TPB + m
                tile = tile_of(at)
                if ready:
                    table = inner_ref[at]
                    cosine, sine = outer_ref[at, s, 0], outer_ref[at, s, 1]
                else:
                    band = band_of(slot) + bin_half * bands_half
                    lag, table = inner_tables(tile, lags_ref, inner_at)
                    turn = (band.astype(jnp.float32) + 0.5) / (2 * bands_half) * time
                    frequency = (band * width).astype(jnp.float32) + start_at
                    cosine, sine = outer_tables(tile, lag, drift_ref, turn, frequency, live)
                rhs = jnp.concatenate([table[:INNER], table], 0)
                product = jnp.dot(lhs, rhs, preferred_element_type=jnp.float32)
                terms = jnp.sum(cosine * product[:outer] - sine * product[outer:], axis=0, keepdims=True)
                total[s, tile] += jnp.concatenate([terms[:, c * LANES : (c + 1) * LANES] for c in range(per_tile)], 0)

        over_slots(slots, one_slot)
        tiles = rows_dest // per_tile
        powers = jnp.concatenate(powers, 0)
        for d in range(dests):
            piece = total[s, d * tiles : (d + 1) * tiles].reshape(rows_dest, LANES)
            out_ref[d, s] = jnp.concatenate([piece, powers], 0).astype(jnp.bfloat16)


def weights_of(power, fourier_bins):
    halves = power[..., 0::2, :] + power[..., 1::2, :]
    whole = halves.reshape(2, 2, *halves.shape[1:]).sum(1) / fourier_bins + 1e-06
    return 1.0 / (whole[..., 0, :] * whole[..., 1, :])


def sum_kernel(tm_count, rows_dest, fourier_bins, scale, got_ref, out_ref):
    seg_kept = got_ref.shape[1]
    total = jnp.zeros((rows_dest, LANES), jnp.float32)
    for k in range(2):
        for i in range(tm_count):
            for s in range(seg_kept):
                pair = [got_ref[(2 * k + h) * tm_count + i, s].astype(jnp.float32) for h in range(2)]
                both = pair[0] + pair[1]
                own = (both[rows_dest : rows_dest + 1] + both[rows_dest + 1 : rows_dest + 2]) / fourier_bins + 1e-06
                other = (both[rows_dest + 2 : rows_dest + 3] + both[rows_dest + 3 : rows_dest + 4]) / fourier_bins + 1e-06
                total = total + both[:rows_dest] * (1.0 / (own * other))
    out_ref[...] = total / scale


def shards(spectra, valid, lags, drift, block_table):
    det_count, tm_count = lax.axis_size("det"), lax.axis_size("tm")
    devices = det_count * tm_count
    own = spectra[0]
    seg_count, bands_half, _, width = own.shape
    seg_kept = seg_count // 2
    pixels = lags.shape[0]
    per_device = pixels // devices
    fourier_bins = 2 * bands_half * width
    scale = math.sqrt(seg_count * tm_count * width)
    direct = per_device % PT == 0
    rows_dest = (per_device if direct else pixels) // LANES
    dests = devices if direct else 1
    rows = rows_dest + 4
    per_tile = PT // LANES
    blocks = block_table.shape[0] // 2
    slots = blocks // TPB
    outer = width // INNER

    own = own.reshape(seg_count, 2 * bands_half, width)
    other = lax.ppermute(own, "det", [(d, d ^ 3) for d in range(det_count)])
    own = lax.ppermute(own, "det", [(d, d ^ 1) for d in range(det_count)])
    table = block_table.T
    lags, drift = (x.reshape(-1, per_tile, LANES) for x in (lags, drift))
    settings = tuple(pltpu.with_memory_space_constraint(x, pltpu.HBM) for x in (valid, table, lags, drift))
    held = [pltpu.SMEM(valid.shape, jnp.int32), pltpu.SMEM(table.shape, jnp.int32)]
    held += [pltpu.VMEM(lags.shape, jnp.float32), pltpu.VMEM(drift.shape, jnp.float32)]
    work = [pltpu.VMEM(own.shape[1:], jnp.float32), pltpu.VMEM((slots, 2 * outer, width), jnp.bfloat16)]
    mixed = jax.ShapeDtypeStruct((seg_kept, 8, slots, outer, LANES), jnp.float32)
    ready = slots <= UNROLLED
    if ready:
        made = pl.pallas_call(
            functools.partial(tables_kernel, tm_count, bands_half, width, seg_kept),
            out_shape=[
                jax.ShapeDtypeStruct((blocks, 2 * INNER, PT), jnp.bfloat16),
                jax.ShapeDtypeStruct((blocks, seg_kept, 2, outer, PT), jnp.float32),
                jax.ShapeDtypeStruct((slots + blocks, LANES), jnp.int32),
            ],
            in_specs=[HBM] * 4,
            out_specs=[VMEM] * 3,
            scratch_shapes=[*held, pltpu.SemaphoreType.DMA((4,))],
            compiler_params=GRANT,
            cost_estimate=pl.CostEstimate(flops=10**9, bytes_accessed=10**6, transcendentals=0),
            name="tables",
        )(*settings)
        factors = pl.pallas_call(
            functools.partial(mix_kernel, seg_kept),
            out_shape=[mixed, jax.ShapeDtypeStruct((seg_kept, 2, LANES), jnp.float32)],
            in_specs=[VMEM] * 2,
            out_specs=[VMEM] * 2,
            scratch_shapes=work,
            compiler_params=GRANT,
            cost_estimate=pl.CostEstimate(flops=10**8, bytes_accessed=10**6, transcendentals=0),
            name="mix",
        )(made[2], own)
        settings, held = (*made, *factors), []
    else:
        settings = (*settings, own)
        held += [pltpu.SemaphoreType.DMA((4,)), pltpu.VMEM(mixed.shape, mixed.dtype)]
    outgoing = pl.pallas_call(
        functools.partial(terms_kernel, tm_count, dests, rows_dest, seg_kept, ready),
        out_shape=jax.ShapeDtypeStruct((dests, seg_kept, rows, LANES), jnp.bfloat16),
        in_specs=([VMEM] * 5 if ready else [HBM] * 4 + [VMEM]) + [VMEM],
        out_specs=VMEM,
        scratch_shapes=[
            *held,
            *work,
            pltpu.VMEM((slots, 2 * outer, LANES), jnp.bfloat16),
            pltpu.VMEM((seg_kept, pixels // PT, per_tile, LANES), jnp.float32),
        ],
        compiler_params=GRANT if ready else None,
        name="terms",
    )(*settings, other)
    if direct:
        received = lax.all_to_all(outgoing, ("det", "tm"), 0, 0, tiled=True)
        result = pl.pallas_call(
            functools.partial(sum_kernel, tm_count, rows_dest, fourier_bins, scale),
            out_shape=jax.ShapeDtypeStruct((rows_dest, LANES), jnp.float32),
            in_specs=[VMEM],
            out_specs=VMEM,
            compiler_params=GRANT,
            name="sum",
        )(received)
        return result.reshape(-1)
    maps = jnp.moveaxis(outgoing[0, :, :rows_dest].reshape(seg_kept, devices, per_device), 1, 0)
    powers = jnp.broadcast_to(outgoing[0, :, rows_dest : rows_dest + 4, 0], (devices, seg_kept, 4))
    sent = jnp.concatenate([maps, powers], 2)
    received = lax.all_to_all(sent, ("det", "tm"), 0, 0, tiled=True).astype(jnp.float32)
    received = received.reshape(det_count, tm_count, seg_kept, per_device + 4)
    weight = weights_of(received[..., per_device:, None], fourier_bins)[..., 0]
    both = received[..., :per_device].reshape(2, 2, tm_count, seg_kept, per_device).sum(1)
    return (both * weight[..., None]).sum((0, 1, 2)) / scale


def solution(mesh):
    placed = (P("det", "tm", None, None, None), P("tm"), P(), P(), P())
    return jax.shard_map(
        shards, mesh=mesh, in_specs=placed, out_specs=P(("det", "tm")), check_vma=False
    )
```

```python
import functools
import math

import jax
import jax.numpy as jnp
import numpy as np
from jax import lax
from jax.experimental import pallas as pl
from jax.experimental.pallas import tpu as pltpu
from jax.sharding import PartitionSpec as P


PT = 512
TPB = 2
LANES = 128
INNER = 16
HALF = INNER // 2
PARTS = 6
UNROLLED = 16
GRANT = pltpu.CompilerParams(vmem_limit_bytes=8 << 20)

VMEM = pl.BlockSpec(memory_space=pltpu.VMEM)
HBM = pl.BlockSpec(memory_space=pltpu.HBM)


def fitted(function, limit, degree):
    nodes = (np.cos(np.pi * (np.arange(400) + 0.5) / 400) + 1) / 2
    powers = np.vander(nodes, degree + 1, increasing=True)
    coefficients = np.linalg.lstsq(powers, function(np.sqrt(nodes * limit)), rcond=None)[0]
    return tuple(float(c) for c in coefficients / limit ** np.arange(degree + 1))


NEAR_COS = fitted(lambda r: np.cos(2 * np.pi * r), 0.0064, 3)
NEAR_SIN = fitted(lambda r: np.sin(2 * np.pi * r) / r, 0.0064, 3)
FAR_COS = fitted(lambda r: np.cos(2 * np.pi * r), 0.25, 6)
FAR_SIN = fitted(lambda r: np.sin(2 * np.pi * r) / r, 0.25, 6)


def horner(coefficients, z):
    total = jnp.full_like(z, coefficients[-1])
    for c in coefficients[-2::-1]:
        total = total * z + c
    return total


def near_turn(x):
    z = x * x
    return horner(NEAR_COS, z), x * horner(NEAR_SIN, z)


def any_turn(x):
    r = x - jnp.floor(x + 0.5)
    z = r * r
    return horner(FAR_COS, z), r * horner(FAR_SIN, z)


def split(x):
    high = x.astype(jnp.bfloat16)
    return high, (x - high.astype(jnp.float32)).astype(jnp.bfloat16)


def block_of(slot, table_ref, tm_count, bin_half):
    per_group = table_ref.shape[1] // (2 * tm_count)
    first = slot * TPB
    return (2 * (first // per_group) + bin_half) * per_group + first % per_group


def over_slots(slots, one_slot):
    if slots <= UNROLLED:
        for slot in range(slots):
            one_slot(slot)
    else:
        lax.fori_loop(0, slots, lambda slot, _: (one_slot(slot), 0)[1], 0)


def inner_tables(tile, lags_ref, inner_at):
    lag = jnp.concatenate([lags_ref[tile, c : c + 1, :] for c in range(PT // LANES)], 1)
    cosine, sine = near_turn(jnp.broadcast_to(lag, inner_at.shape) * inner_at)
    return lag, jnp.concatenate(split(jnp.concatenate([cosine, sine], 0)), 0)


def outer_tables(tile, lag, drift_ref, turn, frequency, live):
    pace = jnp.concatenate([drift_ref[tile, c : c + 1, :] for c in range(PT // LANES)], 1)
    shape = frequency.shape
    cosine, sine = any_turn(jnp.broadcast_to(pace * turn, shape) - frequency * jnp.broadcast_to(lag, shape))
    return cosine * live, sine * live


def duty():
    det_index = lax.axis_index("det")
    return 1 - det_index % 2, det_index // 2


def clock(valid_ref, tm_count, detector_bit, seg_kept):
    tm_index = lax.axis_index("tm")
    seg_count = valid_ref.shape[0]
    segment_total = seg_count * tm_count
    marks = []
    for s in range(seg_kept):
        seg = detector_bit * seg_kept + s
        time = ((tm_index * seg_count + seg).astype(jnp.float32) + 0.5 - segment_total / 2) / segment_total
        marks.append((valid_ref[seg].astype(jnp.float32), time))
    return marks


def fetch(sources, targets, sems):
    copies = [pltpu.make_async_copy(a, b, sems.at[n]) for n, (a, b) in enumerate(zip(sources, targets))]
    for copy in copies:
        copy.start()
    return copies


def start_rows(outer):
    return (lax.broadcasted_iota(jnp.int32, (outer, PT), 0) * INNER).astype(jnp.float32) + (INNER - 1) / 2


def inner_rows():
    return lax.broadcasted_iota(jnp.int32, (HALF, PT), 0).astype(jnp.float32) + 0.5


def spread(rows_ref, band_of, masked, outer, width, gather=False):
    lane_at = lax.broadcasted_iota(jnp.int32, (outer, width), 1)
    mask = (lane_at // INNER == lax.broadcasted_iota(jnp.int32, (outer, width), 0)).astype(jnp.float32)
    from_lane = lax.broadcasted_iota(jnp.int32, (width, LANES), 0) % INNER
    to_lane = lax.broadcasted_iota(jnp.int32, (width, LANES), 1) % HALF
    choose = jnp.concatenate([from_lane == HALF + to_lane, from_lane == HALF - 1 - to_lane], 1)

    def one_slot(slot):
        row = 2 * band_of(slot)
        pair = [jnp.broadcast_to(rows_ref[pl.ds(row + c, 1), :], (outer, width)) * mask for c in range(2)]
        return jnp.concatenate(pair, 0).astype(jnp.bfloat16)

    slots = masked.shape[0]
    if slots <= UNROLLED and gather:
        at = lax.broadcasted_iota(jnp.int32, (outer, LANES), 0) * INNER
        lane = lax.broadcasted_iota(jnp.int32, (outer, LANES), 1) % HALF
        sources = (at + HALF + lane, at + HALF - 1 - lane)
        rows = [[jnp.broadcast_to(rows_ref[pl.ds(2 * band_of(slot) + c, 1), :], (outer, width)) for c in range(2)] for slot in range(slots)]
        return [
            jnp.stack([jnp.take_along_axis(pair[c], source, axis=1, mode="promise_in_bounds") for pair in rows])
            for source in sources
            for c in range(2)
        ]
    if slots <= UNROLLED:
        stacked = jnp.concatenate([one_slot(slot) for slot in range(slots)], 0)
    else:
        def kept(slot):
            masked[slot] = one_slot(slot)

        over_slots(slots, kept)
        stacked = masked[...].reshape(slots * 2 * outer, width)
    wide = jnp.dot(stacked, choose.astype(jnp.float32).astype(jnp.bfloat16), preferred_element_type=jnp.float32)
    wide = wide.reshape(slots, 2 * outer, 2 * LANES)
    return [wide[:, c * outer : (c + 1) * outer, m * LANES : (m + 1) * LANES] for m in range(2) for c in range(2)]


def mix_own(rows_ref, band_of, masked, mixed_ref, s, flip, outer, width):
    real, imag, real_m, imag_m = spread(rows_ref, band_of, masked, outer, width)
    even = lax.broadcasted_iota(jnp.int32, real.shape, 2) // HALF % 2 == 0
    turned, turned_m = flip * imag, flip * imag_m
    kept, kept_m = flip * real, flip * real_m
    factors = (
        (real, -turned), (imag, kept), (real_m, turned_m), (imag_m, -kept_m),
        (-turned, -real), (kept, -imag), (-turned_m, real_m), (kept_m, imag_m),
    )
    for n, (first, second) in enumerate(factors):
        mixed_ref[s, n] = jnp.where(even, first, second)


def power_rows(rows):
    power = jnp.sum(jnp.sum(rows * rows, axis=0, keepdims=True), axis=1, keepdims=True)
    high = power.astype(jnp.bfloat16).astype(jnp.float32)
    return jnp.concatenate([jnp.broadcast_to(x, (1, LANES)) for x in (high, power - high)], 0)


def tables_kernel(
    tm_count, bands_half, width, seg_kept,
    valid_hbm, table_hbm, lags_hbm, drift_hbm,
    inner_ref, outer_ref, picks_ref,
    valid_ref, table_ref, lags_ref, drift_ref, sems,
):
    bin_half, detector_bit = duty()
    copies = fetch((valid_hbm, table_hbm, lags_hbm, drift_hbm), (valid_ref, table_ref, lags_ref, drift_ref), sems)
    inner_at, start_at = inner_rows(), start_rows(width // INNER)
    for copy in copies:
        copy.wait()
    marks = clock(valid_ref, tm_count, detector_bit, seg_kept)

    def one_slot(slot):
        row = block_of(slot, table_ref, tm_count, bin_half)
        band = table_ref[0, row]
        frequency = (band * width).astype(jnp.float32) + start_at
        share = (band.astype(jnp.float32) + 0.5) / (2 * bands_half)
        picks_ref[slot : slot + 1, :] = jnp.full((1, LANES), band - bin_half * bands_half)
        for m in range(TPB):
            tile = table_ref[1, row + m]
            at = slot * TPB + m
            picks_ref[slots + at : slots + at + 1, :] = jnp.full((1, LANES), tile)
            lag, parts = inner_tables(tile, lags_ref, inner_at)
            inner_ref[at] = parts
            for s, (live, time) in enumerate(marks):
                cosine, sine = outer_tables(tile, lag, drift_ref, share * time, frequency, live)
                outer_ref[at, s, 0] = cosine
                outer_ref[at, s, 1] = sine

    slots = inner_ref.shape[0] // TPB
    over_slots(slots, one_slot)


def mix_kernel(seg_kept, picks_ref, own_ref, mixed_ref, power_ref, rows32, masked):
    _, detector_bit = duty()
    _, outer = mixed_ref.shape[2:4]
    flip = jnp.where(detector_bit == 0, 1.0, -1.0).astype(jnp.float32)

    def band_of(slot):
        return picks_ref[slot : slot + 1, :][0, 0]

    for s in range(seg_kept):
        rows32[...] = own_ref[detector_bit * seg_kept + s].astype(jnp.float32)
        power_ref[s] = power_rows(rows32[...])
        mix_own(rows32, band_of, masked, mixed_ref, s, flip, outer, own_ref.shape[2])


def terms_kernel(tm_count, dests, rows_dest, seg_kept, ready, *refs):
    if ready:
        inner_ref, outer_ref, picks_ref, mixed_ref, power_ref, other_ref, out_ref, *scratch = refs
        copies = ()
    else:
        valid_hbm, table_hbm, lags_hbm, drift_hbm, own_ref, other_ref, out_ref, *scratch = refs
        valid_ref, table_ref, lags_ref, drift_ref, sems, mixed_ref, *scratch = scratch
        copies = fetch((valid_hbm, table_hbm, lags_hbm, drift_hbm), (valid_ref, table_ref, lags_ref, drift_ref), sems)
    rows32, masked, left, total = scratch
    bin_half, detector_bit = duty()
    bands_half = other_ref.shape[1] // 2
    width = other_ref.shape[2]
    outer = width // INNER
    per_tile = PT // LANES
    slots = masked.shape[0]
    flip = jnp.where(detector_bit == 0, 1.0, -1.0).astype(jnp.float32)
    part = lax.broadcasted_iota(jnp.int32, (slots, outer, LANES), 2) // HALF
    total[...] = jnp.zeros_like(total)

    def band_of(slot):
        if ready:
            return picks_ref[slot : slot + 1, :][0, 0]
        return table_ref[0, block_of(slot, table_ref, tm_count, bin_half)] - bin_half * bands_half

    def tile_of(at):
        if ready:
            return picks_ref[slots + at : slots + at + 1, :][0, 0]
        return table_ref[1, block_of(at // TPB, table_ref, tm_count, bin_half) + at % TPB]

    for s in range(seg_kept):
        seg = detector_bit * seg_kept + s
        rows32[...] = other_ref[seg].astype(jnp.float32)
        powers = [power_ref[s] if ready else power_rows(own_ref[seg].astype(jnp.float32)), power_rows(rows32[...])]
        if s == 0:
            for copy in copies:
                copy.wait()
        wide = spread(rows32, band_of, masked, outer, width, gather=ready)
        if not ready:
            rows32[...] = own_ref[seg].astype(jnp.float32)
            mix_own(rows32, band_of, masked, mixed_ref, s, flip, outer, width)
            inner_at, start_at = inner_rows(), start_rows(outer)
            live, time = clock(valid_ref, tm_count, detector_bit, seg_kept)[s]
        sides = []
        for n in range(2):
            value = sum(mixed_ref[s, 4 * n + q] * wide[q] for q in range(4))
            high = value.astype(jnp.bfloat16).astype(jnp.float32)
            sides.append(jnp.where((part == 2) | (part == 3), value - high, high))
        left[...] = jnp.concatenate(sides, 1).astype(jnp.bfloat16)

        def one_slot(slot):
            lhs = left[slot][:, : PARTS * HALF]
            for m in range(TPB):
                at = slot * TPB + m
                tile = tile_of(at)
                if ready:
                    table = inner_ref[at]
                    cosine, sine = outer_ref[at, s, 0], outer_ref[at, s, 1]
                else:
                    band = band_of(slot) + bin_half * bands_half
                    lag, table = inner_tables(tile, lags_ref, inner_at)
                    turn = (band.astype(jnp.float32) + 0.5) / (2 * bands_half) * time
                    frequency = (band * width).astype(jnp.float32) + start_at
                    cosine, sine = outer_tables(tile, lag, drift_ref, turn, frequency, live)
                rhs = jnp.concatenate([table[:INNER], table], 0)
                product = jnp.dot(lhs, rhs, preferred_element_type=jnp.float32)
                terms = jnp.sum(cosine * product[:outer] - sine * product[outer:], axis=0, keepdims=True)
                total[s, tile] += jnp.concatenate([terms[:, c * LANES : (c + 1) * LANES] for c in range(per_tile)], 0)

        over_slots(slots, one_slot)
        tiles = rows_dest // per_tile
        powers = jnp.concatenate(powers, 0)
        for d in range(dests):
            piece = total[s, d * tiles : (d + 1) * tiles].reshape(rows_dest, LANES)
            out_ref[d, s] = jnp.concatenate([piece, powers], 0).astype(jnp.bfloat16)


def weights_of(power, fourier_bins):
    halves = power[..., 0::2, :] + power[..., 1::2, :]
    whole = halves.reshape(2, 2, *halves.shape[1:]).sum(1) / fourier_bins + 1e-06
    return 1.0 / (whole[..., 0, :] * whole[..., 1, :])


def sum_kernel(tm_count, rows_dest, fourier_bins, scale, got_ref, out_ref):
    seg_kept = got_ref.shape[1]
    total = jnp.zeros((rows_dest, LANES), jnp.float32)
    for k in range(2):
        for i in range(tm_count):
            for s in range(seg_kept):
                pair = [got_ref[(2 * k + h) * tm_count + i, s].astype(jnp.float32) for h in range(2)]
                both = pair[0] + pair[1]
                own = (both[rows_dest : rows_dest + 1] + both[rows_dest + 1 : rows_dest + 2]) / fourier_bins + 1e-06
                other = (both[rows_dest + 2 : rows_dest + 3] + both[rows_dest + 3 : rows_dest + 4]) / fourier_bins + 1e-06
                total = total + both[:rows_dest] * (1.0 / (own * other))
    out_ref[...] = total / scale


def shards(spectra, valid, lags, drift, block_table):
    det_count, tm_count = lax.axis_size("det"), lax.axis_size("tm")
    devices = det_count * tm_count
    own = spectra[0]
    seg_count, bands_half, _, width = own.shape
    seg_kept = seg_count // 2
    pixels = lags.shape[0]
    per_device = pixels // devices
    fourier_bins = 2 * bands_half * width
    scale = math.sqrt(seg_count * tm_count * width)
    direct = per_device % PT == 0
    rows_dest = (per_device if direct else pixels) // LANES
    dests = devices if direct else 1
    rows = rows_dest + 4
    per_tile = PT // LANES
    blocks = block_table.shape[0] // 2
    slots = blocks // TPB
    outer = width // INNER

    own = own.reshape(seg_count, 2 * bands_half, width)
    other = lax.ppermute(own, "det", [(d, d ^ 3) for d in range(det_count)])
    own = lax.ppermute(own, "det", [(d, d ^ 1) for d in range(det_count)])
    table = block_table.T
    lags, drift = (x.reshape(-1, per_tile, LANES) for x in (lags, drift))
    settings = tuple(pltpu.with_memory_space_constraint(x, pltpu.HBM) for x in (valid, table, lags, drift))
    held = [pltpu.SMEM(valid.shape, jnp.int32), pltpu.SMEM(table.shape, jnp.int32)]
    held += [pltpu.VMEM(lags.shape, jnp.float32), pltpu.VMEM(drift.shape, jnp.float32)]
    work = [pltpu.VMEM(own.shape[1:], jnp.float32), pltpu.VMEM((slots, 2 * outer, width), jnp.bfloat16)]
    mixed = jax.ShapeDtypeStruct((seg_kept, 8, slots, outer, LANES), jnp.float32)
    ready = slots <= UNROLLED
    if ready:
        made = pl.pallas_call(
            functools.partial(tables_kernel, tm_count, bands_half, width, seg_kept),
            out_shape=[
                jax.ShapeDtypeStruct((blocks, 2 * INNER, PT), jnp.bfloat16),
                jax.ShapeDtypeStruct((blocks, seg_kept, 2, outer, PT), jnp.float32),
                jax.ShapeDtypeStruct((slots + blocks, LANES), jnp.int32),
            ],
            in_specs=[HBM] * 4,
            out_specs=[VMEM] * 3,
            scratch_shapes=[*held, pltpu.SemaphoreType.DMA((4,))],
            compiler_params=GRANT,
            cost_estimate=pl.CostEstimate(flops=10**9, bytes_accessed=10**6, transcendentals=0),
            name="tables",
        )(*settings)
        factors = pl.pallas_call(
            functools.partial(mix_kernel, seg_kept),
            out_shape=[mixed, jax.ShapeDtypeStruct((seg_kept, 2, LANES), jnp.float32)],
            in_specs=[VMEM] * 2,
            out_specs=[VMEM] * 2,
            scratch_shapes=work,
            compiler_params=GRANT,
            cost_estimate=pl.CostEstimate(flops=10**8, bytes_accessed=10**6, transcendentals=0),
            name="mix",
        )(made[2], own)
        settings, held = (*made, *factors), []
    else:
        settings = (*settings, own)
        held += [pltpu.SemaphoreType.DMA((4,)), pltpu.VMEM(mixed.shape, mixed.dtype)]
    outgoing = pl.pallas_call(
        functools.partial(terms_kernel, tm_count, dests, rows_dest, seg_kept, ready),
        out_shape=jax.ShapeDtypeStruct((dests, seg_kept, rows, LANES), jnp.bfloat16),
        in_specs=([VMEM] * 5 if ready else [HBM] * 4 + [VMEM]) + [VMEM],
        out_specs=VMEM,
        scratch_shapes=[
            *held,
            *work,
            pltpu.VMEM((slots, 2 * outer, LANES), jnp.bfloat16),
            pltpu.VMEM((seg_kept, pixels // PT, per_tile, LANES), jnp.float32),
        ],
        compiler_params=GRANT if ready else None,
        name="terms",
    )(*settings, other)
    if direct:
        received = lax.all_to_all(outgoing, ("det", "tm"), 0, 0, tiled=True)
        result = pl.pallas_call(
            functools.partial(sum_kernel, tm_count, rows_dest, fourier_bins, scale),
            out_shape=jax.ShapeDtypeStruct((rows_dest, LANES), jnp.float32),
            in_specs=[VMEM],
            out_specs=VMEM,
            compiler_params=GRANT,
            name="sum",
        )(received)
        return result.reshape(-1)
    maps = jnp.moveaxis(outgoing[0, :, :rows_dest].reshape(seg_kept, devices, per_device), 1, 0)
    powers = jnp.broadcast_to(outgoing[0, :, rows_dest : rows_dest + 4, 0], (devices, seg_kept, 4))
    sent = jnp.concatenate([maps, powers], 2)
    received = lax.all_to_all(sent, ("det", "tm"), 0, 0, tiled=True).astype(jnp.float32)
    received = received.reshape(det_count, tm_count, seg_kept, per_device + 4)
    weight = weights_of(received[..., per_device:, None], fourier_bins)[..., 0]
    both = received[..., :per_device].reshape(2, 2, tm_count, seg_kept, per_device).sum(1)
    return (both * weight[..., None]).sum((0, 1, 2)) / scale


def solution(mesh):
    placed = (P("det", "tm", None, None, None), P("tm"), P(), P(), P())
    return jax.shard_map(
        shards, mesh=mesh, in_specs=placed, out_specs=P(("det", "tm")), check_vma=False
    )
```

```python
import functools
import math

import jax
import jax.numpy as jnp
import numpy as np
from jax import lax
from jax.experimental import pallas as pl
from jax.experimental.pallas import tpu as pltpu
from jax.sharding import PartitionSpec as P


PT = 512
TPB = 2
LANES = 128
INNER = 16
HALF = INNER // 2
PARTS = 6
UNROLLED = 16
GRANT = pltpu.CompilerParams(vmem_limit_bytes=8 << 20)

VMEM = pl.BlockSpec(memory_space=pltpu.VMEM)
HBM = pl.BlockSpec(memory_space=pltpu.HBM)


def fitted(function, limit, degree):
    nodes = (np.cos(np.pi * (np.arange(400) + 0.5) / 400) + 1) / 2
    powers = np.vander(nodes, degree + 1, increasing=True)
    coefficients = np.linalg.lstsq(powers, function(np.sqrt(nodes * limit)), rcond=None)[0]
    return tuple(float(c) for c in coefficients / limit ** np.arange(degree + 1))


NEAR_COS = fitted(lambda r: np.cos(2 * np.pi * r), 0.0064, 3)
NEAR_SIN = fitted(lambda r: np.sin(2 * np.pi * r) / r, 0.0064, 3)
FAR_COS = fitted(lambda r: np.cos(2 * np.pi * r), 0.25, 6)
FAR_SIN = fitted(lambda r: np.sin(2 * np.pi * r) / r, 0.25, 6)


def horner(coefficients, z):
    total = jnp.full_like(z, coefficients[-1])
    for c in coefficients[-2::-1]:
        total = total * z + c
    return total


def near_turn(x):
    z = x * x
    return horner(NEAR_COS, z), x * horner(NEAR_SIN, z)


def any_turn(x):
    r = x - jnp.floor(x + 0.5)
    z = r * r
    return horner(FAR_COS, z), r * horner(FAR_SIN, z)


def split(x):
    high = x.astype(jnp.bfloat16)
    return high, (x - high.astype(jnp.float32)).astype(jnp.bfloat16)


def block_of(slot, table_ref, tm_count, bin_half):
    per_group = table_ref.shape[1] // (2 * tm_count)
    first = slot * TPB
    return (2 * (first // per_group) + bin_half) * per_group + first % per_group


def over_slots(slots, one_slot):
    if slots <= UNROLLED:
        for slot in range(slots):
            one_slot(slot)
    else:
        lax.fori_loop(0, slots, lambda slot, _: (one_slot(slot), 0)[1], 0)


def inner_tables(tile, lags_ref, inner_at):
    lag = jnp.concatenate([lags_ref[tile, c : c + 1, :] for c in range(PT // LANES)], 1)
    cosine, sine = near_turn(jnp.broadcast_to(lag, inner_at.shape) * inner_at)
    return lag, jnp.concatenate(split(jnp.concatenate([cosine, sine], 0)), 0)


def outer_tables(tile, lag, drift_ref, turn, frequency, live):
    pace = jnp.concatenate([drift_ref[tile, c : c + 1, :] for c in range(PT // LANES)], 1)
    shape = frequency.shape
    cosine, sine = any_turn(jnp.broadcast_to(pace * turn, shape) - frequency * jnp.broadcast_to(lag, shape))
    return cosine * live, sine * live


def duty():
    det_index = lax.axis_index("det")
    return 1 - det_index % 2, det_index // 2


def clock(valid_ref, tm_count, detector_bit, seg_kept):
    tm_index = lax.axis_index("tm")
    seg_count = valid_ref.shape[0]
    segment_total = seg_count * tm_count
    marks = []
    for s in range(seg_kept):
        seg = detector_bit * seg_kept + s
        time = ((tm_index * seg_count + seg).astype(jnp.float32) + 0.5 - segment_total / 2) / segment_total
        marks.append((valid_ref[seg].astype(jnp.float32), time))
    return marks


def fetch(sources, targets, sems):
    copies = [pltpu.make_async_copy(a, b, sems.at[n]) for n, (a, b) in enumerate(zip(sources, targets))]
    for copy in copies:
        copy.start()
    return copies


def start_rows(outer):
    return (lax.broadcasted_iota(jnp.int32, (outer, PT), 0) * INNER).astype(jnp.float32) + (INNER - 1) / 2


def inner_rows():
    return lax.broadcasted_iota(jnp.int32, (HALF, PT), 0).astype(jnp.float32) + 0.5


def spread(rows_ref, band_of, masked, outer, width, gather=False):
    lane_at = lax.broadcasted_iota(jnp.int32, (outer, width), 1)
    mask = (lane_at // INNER == lax.broadcasted_iota(jnp.int32, (outer, width), 0)).astype(jnp.float32)
    from_lane = lax.broadcasted_iota(jnp.int32, (width, LANES), 0) % INNER
    to_lane = lax.broadcasted_iota(jnp.int32, (width, LANES), 1) % HALF
    choose = jnp.concatenate([from_lane == HALF + to_lane, from_lane == HALF - 1 - to_lane], 1)

    def one_slot(slot):
        row = 2 * band_of(slot)
        pair = [jnp.broadcast_to(rows_ref[pl.ds(row + c, 1), :], (outer, width)) * mask for c in range(2)]
        return jnp.concatenate(pair, 0).astype(jnp.bfloat16)

    slots = masked.shape[0]
    if slots <= UNROLLED and gather:
        at = lax.broadcasted_iota(jnp.int32, (outer, LANES), 0) * INNER
        lane = lax.broadcasted_iota(jnp.int32, (outer, LANES), 1) % HALF
        sources = (at + HALF + lane, at + HALF - 1 - lane)
        found = []
        for slot in range(slots):
            row = 2 * band_of(slot)
            pair = [jnp.broadcast_to(rows_ref[pl.ds(row + c, 1), :], (outer, width)) for c in range(2)]
            found.append([jnp.take_along_axis(x, source, axis=1, mode="promise_in_bounds") for source in sources for x in pair])
        return [jnp.stack(wide) for wide in zip(*found)]
    if slots <= UNROLLED:
        stacked = jnp.concatenate([one_slot(slot) for slot in range(slots)], 0)
    else:
        def kept(slot):
            masked[slot] = one_slot(slot)

        over_slots(slots, kept)
        stacked = masked[...].reshape(slots * 2 * outer, width)
    wide = jnp.dot(stacked, choose.astype(jnp.float32).astype(jnp.bfloat16), preferred_element_type=jnp.float32)
    wide = wide.reshape(slots, 2 * outer, 2 * LANES)
    return [wide[:, c * outer : (c + 1) * outer, m * LANES : (m + 1) * LANES] for m in range(2) for c in range(2)]


def mix_own(rows_ref, band_of, masked, mixed_ref, s, flip, outer, width):
    real, imag, real_m, imag_m = spread(rows_ref, band_of, masked, outer, width)
    even = lax.broadcasted_iota(jnp.int32, real.shape, 2) // HALF % 2 == 0
    turned, turned_m = flip * imag, flip * imag_m
    kept, kept_m = flip * real, flip * real_m
    factors = (
        (real, -turned), (imag, kept), (real_m, turned_m), (imag_m, -kept_m),
        (-turned, -real), (kept, -imag), (-turned_m, real_m), (kept_m, imag_m),
    )
    for n, (first, second) in enumerate(factors):
        mixed_ref[s, n] = jnp.where(even, first, second)


def power_rows(rows):
    power = jnp.sum(jnp.sum(rows * rows, axis=0, keepdims=True), axis=1, keepdims=True)
    high = power.astype(jnp.bfloat16).astype(jnp.float32)
    return jnp.concatenate([jnp.broadcast_to(x, (1, LANES)) for x in (high, power - high)], 0)


def tables_kernel(
    tm_count, bands_half, width, seg_kept,
    valid_hbm, table_hbm, lags_hbm, drift_hbm,
    inner_ref, outer_ref, picks_ref,
    valid_ref, table_ref, lags_ref, drift_ref, sems,
):
    bin_half, detector_bit = duty()
    copies = fetch((valid_hbm, table_hbm, lags_hbm, drift_hbm), (valid_ref, table_ref, lags_ref, drift_ref), sems)
    inner_at, start_at = inner_rows(), start_rows(width // INNER)
    for copy in copies:
        copy.wait()
    marks = clock(valid_ref, tm_count, detector_bit, seg_kept)

    def one_slot(slot):
        row = block_of(slot, table_ref, tm_count, bin_half)
        band = table_ref[0, row]
        frequency = (band * width).astype(jnp.float32) + start_at
        share = (band.astype(jnp.float32) + 0.5) / (2 * bands_half)
        picks_ref[slot : slot + 1, :] = jnp.full((1, LANES), band - bin_half * bands_half)
        for m in range(TPB):
            tile = table_ref[1, row + m]
            at = slot * TPB + m
            picks_ref[slots + at : slots + at + 1, :] = jnp.full((1, LANES), tile)
            lag, parts = inner_tables(tile, lags_ref, inner_at)
            inner_ref[at] = parts
            for s, (live, time) in enumerate(marks):
                cosine, sine = outer_tables(tile, lag, drift_ref, share * time, frequency, live)
                outer_ref[at, s, 0] = cosine
                outer_ref[at, s, 1] = sine

    slots = inner_ref.shape[0] // TPB
    over_slots(slots, one_slot)


def mix_kernel(seg_kept, picks_ref, own_ref, mixed_ref, power_ref, rows32, masked):
    _, detector_bit = duty()
    _, outer = mixed_ref.shape[2:4]
    flip = jnp.where(detector_bit == 0, 1.0, -1.0).astype(jnp.float32)

    def band_of(slot):
        return picks_ref[slot : slot + 1, :][0, 0]

    for s in range(seg_kept):
        rows32[...] = own_ref[detector_bit * seg_kept + s].astype(jnp.float32)
        power_ref[s] = power_rows(rows32[...])
        mix_own(rows32, band_of, masked, mixed_ref, s, flip, outer, own_ref.shape[2])


def gathered(terms):
    parts = [terms[:, c * LANES : (c + 1) * LANES] for c in range(PT // LANES)]
    row = lax.broadcasted_iota(jnp.int32, parts[0].shape, 0)
    count, distance = parts[0].shape[0], 1
    while len(parts) > 1:
        first = row // distance % 2 == 0
        parts = [
            jnp.where(first, a, b) + pltpu.roll(jnp.where(first, b, a), count - distance, 0)
            for a, b in zip(parts[::2], parts[1::2])
        ]
        distance *= 2
    while distance < count:
        parts = [parts[0] + pltpu.roll(parts[0], count - distance, 0)]
        distance *= 2
    return parts[0][: PT // LANES]


def terms_kernel(tm_count, dests, rows_dest, seg_kept, ready, *refs):
    if ready:
        inner_ref, outer_ref, picks_ref, mixed_ref, power_ref, other_ref, out_ref, *scratch = refs
        copies = ()
    else:
        valid_hbm, table_hbm, lags_hbm, drift_hbm, own_ref, other_ref, out_ref, *scratch = refs
        valid_ref, table_ref, lags_ref, drift_ref, sems, mixed_ref, *scratch = scratch
        copies = fetch((valid_hbm, table_hbm, lags_hbm, drift_hbm), (valid_ref, table_ref, lags_ref, drift_ref), sems)
    rows32, masked, left, total = scratch
    bin_half, detector_bit = duty()
    bands_half = other_ref.shape[1] // 2
    width = other_ref.shape[2]
    outer = width // INNER
    per_tile = PT // LANES
    slots = masked.shape[0]
    flip = jnp.where(detector_bit == 0, 1.0, -1.0).astype(jnp.float32)
    part = lax.broadcasted_iota(jnp.int32, (slots, outer, LANES), 2) // HALF
    total[...] = jnp.zeros_like(total)

    def band_of(slot):
        if ready:
            return picks_ref[slot : slot + 1, :][0, 0]
        return table_ref[0, block_of(slot, table_ref, tm_count, bin_half)] - bin_half * bands_half

    def tile_of(at):
        if ready:
            return picks_ref[slots + at : slots + at + 1, :][0, 0]
        return table_ref[1, block_of(at // TPB, table_ref, tm_count, bin_half) + at % TPB]

    for s in range(seg_kept):
        seg = detector_bit * seg_kept + s
        rows32[...] = other_ref[seg].astype(jnp.float32)
        powers = [power_ref[s] if ready else power_rows(own_ref[seg].astype(jnp.float32)), power_rows(rows32[...])]
        if s == 0:
            for copy in copies:
                copy.wait()
        wide = spread(rows32, band_of, masked, outer, width, gather=ready)
        if not ready:
            rows32[...] = own_ref[seg].astype(jnp.float32)
            mix_own(rows32, band_of, masked, mixed_ref, s, flip, outer, width)
            inner_at, start_at = inner_rows(), start_rows(outer)
            live, time = clock(valid_ref, tm_count, detector_bit, seg_kept)[s]
        sides = []
        for n in range(2):
            value = sum(mixed_ref[s, 4 * n + q] * wide[q] for q in range(4))
            high = value.astype(jnp.bfloat16).astype(jnp.float32)
            sides.append(jnp.where((part == 2) | (part == 3), value - high, high))
        lefts = jnp.concatenate(sides, 1).astype(jnp.bfloat16)
        if not ready:
            left[...] = lefts

        def one_slot(slot):
            lhs = (lefts if ready else left)[slot][:, : PARTS * HALF]
            for m in range(TPB):
                at = slot * TPB + m
                tile = tile_of(at)
                if ready:
                    table = inner_ref[at]
                    cosine, sine = outer_ref[at, s, 0], outer_ref[at, s, 1]
                else:
                    band = band_of(slot) + bin_half * bands_half
                    lag, table = inner_tables(tile, lags_ref, inner_at)
                    turn = (band.astype(jnp.float32) + 0.5) / (2 * bands_half) * time
                    frequency = (band * width).astype(jnp.float32) + start_at
                    cosine, sine = outer_tables(tile, lag, drift_ref, turn, frequency, live)
                rhs = jnp.concatenate([table[:INNER], table], 0)
                product = jnp.dot(lhs, rhs, preferred_element_type=jnp.float32)
                total[s, tile] += gathered(cosine * product[:outer] - sine * product[outer:])

        over_slots(slots, one_slot)
        tiles = rows_dest // per_tile
        powers = jnp.concatenate(powers, 0)
        for d in range(dests):
            piece = total[s, d * tiles : (d + 1) * tiles].reshape(rows_dest, LANES)
            out_ref[d, s] = jnp.concatenate([piece, powers], 0).astype(jnp.bfloat16)


def weights_of(power, fourier_bins):
    halves = power[..., 0::2, :] + power[..., 1::2, :]
    whole = halves.reshape(2, 2, *halves.shape[1:]).sum(1) / fourier_bins + 1e-06
    return 1.0 / (whole[..., 0, :] * whole[..., 1, :])


def sum_kernel(tm_count, rows_dest, fourier_bins, scale, got_ref, out_ref):
    seg_kept = got_ref.shape[1]
    total = jnp.zeros((rows_dest, LANES), jnp.float32)
    for k in range(2):
        for i in range(tm_count):
            for s in range(seg_kept):
                pair = [got_ref[(2 * k + h) * tm_count + i, s].astype(jnp.float32) for h in range(2)]
                both = pair[0] + pair[1]
                own = (both[rows_dest : rows_dest + 1] + both[rows_dest + 1 : rows_dest + 2]) / fourier_bins + 1e-06
                other = (both[rows_dest + 2 : rows_dest + 3] + both[rows_dest + 3 : rows_dest + 4]) / fourier_bins + 1e-06
                total = total + both[:rows_dest] * (1.0 / (own * other))
    out_ref[...] = total / scale


def shards(spectra, valid, lags, drift, block_table):
    det_count, tm_count = lax.axis_size("det"), lax.axis_size("tm")
    devices = det_count * tm_count
    own = spectra[0]
    seg_count, bands_half, _, width = own.shape
    seg_kept = seg_count // 2
    pixels = lags.shape[0]
    per_device = pixels // devices
    fourier_bins = 2 * bands_half * width
    scale = math.sqrt(seg_count * tm_count * width)
    direct = per_device % PT == 0
    rows_dest = (per_device if direct else pixels) // LANES
    dests = devices if direct else 1
    rows = rows_dest + 4
    per_tile = PT // LANES
    blocks = block_table.shape[0] // 2
    slots = blocks // TPB
    outer = width // INNER

    own = own.reshape(seg_count, 2 * bands_half, width)
    other = lax.ppermute(own, "det", [(d, d ^ 3) for d in range(det_count)])
    own = lax.ppermute(own, "det", [(d, d ^ 1) for d in range(det_count)])
    table = block_table.T
    lags, drift = (x.reshape(-1, per_tile, LANES) for x in (lags, drift))
    settings = tuple(pltpu.with_memory_space_constraint(x, pltpu.HBM) for x in (valid, table, lags, drift))
    held = [pltpu.SMEM(valid.shape, jnp.int32), pltpu.SMEM(table.shape, jnp.int32)]
    held += [pltpu.VMEM(lags.shape, jnp.float32), pltpu.VMEM(drift.shape, jnp.float32)]
    work = [pltpu.VMEM(own.shape[1:], jnp.float32), pltpu.VMEM((slots, 2 * outer, width), jnp.bfloat16)]
    mixed = jax.ShapeDtypeStruct((seg_kept, 8, slots, outer, LANES), jnp.float32)
    ready = slots <= UNROLLED
    if ready:
        made = pl.pallas_call(
            functools.partial(tables_kernel, tm_count, bands_half, width, seg_kept),
            out_shape=[
                jax.ShapeDtypeStruct((blocks, 2 * INNER, PT), jnp.bfloat16),
                jax.ShapeDtypeStruct((blocks, seg_kept, 2, outer, PT), jnp.float32),
                jax.ShapeDtypeStruct((slots + blocks, LANES), jnp.int32),
            ],
            in_specs=[HBM] * 4,
            out_specs=[VMEM] * 3,
            scratch_shapes=[*held, pltpu.SemaphoreType.DMA((4,))],
            compiler_params=GRANT,
            cost_estimate=pl.CostEstimate(flops=10**9, bytes_accessed=10**6, transcendentals=0),
            name="tables",
        )(*settings)
        factors = pl.pallas_call(
            functools.partial(mix_kernel, seg_kept),
            out_shape=[mixed, jax.ShapeDtypeStruct((seg_kept, 2, LANES), jnp.float32)],
            in_specs=[VMEM] * 2,
            out_specs=[VMEM] * 2,
            scratch_shapes=work,
            compiler_params=GRANT,
            cost_estimate=pl.CostEstimate(flops=10**8, bytes_accessed=10**6, transcendentals=0),
            name="mix",
        )(made[2], own)
        settings, held = (*made, *factors), []
    else:
        settings = (*settings, own)
        held += [pltpu.SemaphoreType.DMA((4,)), pltpu.VMEM(mixed.shape, mixed.dtype)]
    outgoing = pl.pallas_call(
        functools.partial(terms_kernel, tm_count, dests, rows_dest, seg_kept, ready),
        out_shape=jax.ShapeDtypeStruct((dests, seg_kept, rows, LANES), jnp.bfloat16),
        in_specs=([VMEM] * 5 if ready else [HBM] * 4 + [VMEM]) + [VMEM],
        out_specs=VMEM,
        scratch_shapes=[
            *held,
            *work,
            pltpu.VMEM((slots, 2 * outer, LANES), jnp.bfloat16),
            pltpu.VMEM((seg_kept, pixels // PT, per_tile, LANES), jnp.float32),
        ],
        compiler_params=GRANT if ready else None,
        name="terms",
    )(*settings, other)
    if direct:
        received = lax.all_to_all(outgoing, ("det", "tm"), 0, 0, tiled=True)
        result = pl.pallas_call(
            functools.partial(sum_kernel, tm_count, rows_dest, fourier_bins, scale),
            out_shape=jax.ShapeDtypeStruct((rows_dest, LANES), jnp.float32),
            in_specs=[VMEM],
            out_specs=VMEM,
            compiler_params=GRANT,
            name="sum",
        )(received)
        return result.reshape(-1)
    maps = jnp.moveaxis(outgoing[0, :, :rows_dest].reshape(seg_kept, devices, per_device), 1, 0)
    powers = jnp.broadcast_to(outgoing[0, :, rows_dest : rows_dest + 4, 0], (devices, seg_kept, 4))
    sent = jnp.concatenate([maps, powers], 2)
    received = lax.all_to_all(sent, ("det", "tm"), 0, 0, tiled=True).astype(jnp.float32)
    received = received.reshape(det_count, tm_count, seg_kept, per_device + 4)
    weight = weights_of(received[..., per_device:, None], fourier_bins)[..., 0]
    both = received[..., :per_device].reshape(2, 2, tm_count, seg_kept, per_device).sum(1)
    return (both * weight[..., None]).sum((0, 1, 2)) / scale


def solution(mesh):
    placed = (P("det", "tm", None, None, None), P("tm"), P(), P(), P())
    return jax.shard_map(
        shards, mesh=mesh, in_specs=placed, out_specs=P(("det", "tm")), check_vma=False
    )
```

```python
import functools
import math

import jax
import jax.numpy as jnp
import numpy as np
from jax import lax
from jax.experimental import pallas as pl
from jax.experimental.pallas import tpu as pltpu
from jax.sharding import PartitionSpec as P


PT = 512
TPB = 2
LANES = 128
INNER = 16
HALF = INNER // 2
PARTS = 6
UNROLLED = 16
GRANT = pltpu.CompilerParams(vmem_limit_bytes=8 << 20)

VMEM = pl.BlockSpec(memory_space=pltpu.VMEM)
HBM = pl.BlockSpec(memory_space=pltpu.HBM)


def fitted(function, limit, degree):
    nodes = (np.cos(np.pi * (np.arange(400) + 0.5) / 400) + 1) / 2
    powers = np.vander(nodes, degree + 1, increasing=True)
    coefficients = np.linalg.lstsq(powers, function(np.sqrt(nodes * limit)), rcond=None)[0]
    return tuple(float(c) for c in coefficients / limit ** np.arange(degree + 1))


NEAR_COS = fitted(lambda r: np.cos(2 * np.pi * r), 0.0064, 3)
NEAR_SIN = fitted(lambda r: np.sin(2 * np.pi * r) / r, 0.0064, 3)
FAR_COS = fitted(lambda r: np.cos(2 * np.pi * r), 0.25, 6)
FAR_SIN = fitted(lambda r: np.sin(2 * np.pi * r) / r, 0.25, 6)


def horner(coefficients, z):
    total = jnp.full_like(z, coefficients[-1])
    for c in coefficients[-2::-1]:
        total = total * z + c
    return total


def near_turn(x):
    z = x * x
    return horner(NEAR_COS, z), x * horner(NEAR_SIN, z)


def any_turn(x):
    r = x - jnp.floor(x + 0.5)
    z = r * r
    return horner(FAR_COS, z), r * horner(FAR_SIN, z)


def split(x):
    high = x.astype(jnp.bfloat16)
    return high, (x - high.astype(jnp.float32)).astype(jnp.bfloat16)


def block_of(slot, table_ref, tm_count, bin_half):
    per_group = table_ref.shape[1] // (2 * tm_count)
    first = slot * TPB
    return (2 * (first // per_group) + bin_half) * per_group + first % per_group


def over_slots(slots, one_slot):
    if slots <= UNROLLED:
        for slot in range(slots):
            one_slot(slot)
    else:
        lax.fori_loop(0, slots, lambda slot, _: (one_slot(slot), 0)[1], 0)


def inner_tables(tile, lags_ref, inner_at):
    lag = jnp.concatenate([lags_ref[tile, c : c + 1, :] for c in range(PT // LANES)], 1)
    cosine, sine = near_turn(jnp.broadcast_to(lag, inner_at.shape) * inner_at)
    return lag, jnp.concatenate(split(jnp.concatenate([cosine, sine], 0)), 0)


def outer_tables(tile, lag, drift_ref, turn, frequency, live):
    pace = jnp.concatenate([drift_ref[tile, c : c + 1, :] for c in range(PT // LANES)], 1)
    shape = frequency.shape
    cosine, sine = any_turn(jnp.broadcast_to(pace * turn, shape) - frequency * jnp.broadcast_to(lag, shape))
    return cosine * live, sine * live


def duty():
    det_index = lax.axis_index("det")
    return 1 - det_index % 2, det_index // 2


def clock(valid_ref, tm_count, detector_bit, seg_kept):
    tm_index = lax.axis_index("tm")
    seg_count = valid_ref.shape[0]
    segment_total = seg_count * tm_count
    marks = []
    for s in range(seg_kept):
        seg = detector_bit * seg_kept + s
        time = ((tm_index * seg_count + seg).astype(jnp.float32) + 0.5 - segment_total / 2) / segment_total
        marks.append((valid_ref[seg].astype(jnp.float32), time))
    return marks


def fetch(sources, targets, sems):
    copies = [pltpu.make_async_copy(a, b, sems.at[n]) for n, (a, b) in enumerate(zip(sources, targets))]
    for copy in copies:
        copy.start()
    return copies


def start_rows(outer):
    return (lax.broadcasted_iota(jnp.int32, (outer, PT), 0) * INNER).astype(jnp.float32) + (INNER - 1) / 2


def inner_rows():
    return lax.broadcasted_iota(jnp.int32, (HALF, PT), 0).astype(jnp.float32) + 0.5


def spread(rows_ref, band_of, masked, outer, width, gather=False):
    lane_at = lax.broadcasted_iota(jnp.int32, (outer, width), 1)
    mask = (lane_at // INNER == lax.broadcasted_iota(jnp.int32, (outer, width), 0)).astype(jnp.float32)
    from_lane = lax.broadcasted_iota(jnp.int32, (width, LANES), 0) % INNER
    to_lane = lax.broadcasted_iota(jnp.int32, (width, LANES), 1) % HALF
    choose = jnp.concatenate([from_lane == HALF + to_lane, from_lane == HALF - 1 - to_lane], 1)

    def one_slot(slot):
        row = 2 * band_of(slot)
        pair = [jnp.broadcast_to(rows_ref[pl.ds(row + c, 1), :], (outer, width)) * mask for c in range(2)]
        return jnp.concatenate(pair, 0).astype(jnp.bfloat16)

    slots = masked.shape[0]
    if slots <= UNROLLED and gather:
        at = lax.broadcasted_iota(jnp.int32, (outer, LANES), 0) * INNER
        lane = lax.broadcasted_iota(jnp.int32, (outer, LANES), 1) % HALF
        sources = (at + HALF + lane, at + HALF - 1 - lane)
        found = []
        for slot in range(slots):
            row = 2 * band_of(slot)
            pair = [jnp.broadcast_to(rows_ref[pl.ds(row + c, 1), :], (outer, width)) for c in range(2)]
            found.append([jnp.take_along_axis(x, source, axis=1, mode="promise_in_bounds") for source in sources for x in pair])
        return [jnp.stack(wide) for wide in zip(*found)]
    if slots <= UNROLLED:
        stacked = jnp.concatenate([one_slot(slot) for slot in range(slots)], 0)
    else:
        def kept(slot):
            masked[slot] = one_slot(slot)

        over_slots(slots, kept)
        stacked = masked[...].reshape(slots * 2 * outer, width)
    wide = jnp.dot(stacked, choose.astype(jnp.float32).astype(jnp.bfloat16), preferred_element_type=jnp.float32)
    wide = wide.reshape(slots, 2 * outer, 2 * LANES)
    return [wide[:, c * outer : (c + 1) * outer, m * LANES : (m + 1) * LANES] for m in range(2) for c in range(2)]


def mix_own(rows_ref, band_of, masked, mixed_ref, s, flip, outer, width):
    real, imag, real_m, imag_m = spread(rows_ref, band_of, masked, outer, width, gather=True)
    even = lax.broadcasted_iota(jnp.int32, real.shape, 2) // HALF % 2 == 0
    turned, turned_m = flip * imag, flip * imag_m
    kept, kept_m = flip * real, flip * real_m
    factors = (
        (real, -turned), (imag, kept), (real_m, turned_m), (imag_m, -kept_m),
        (-turned, -real), (kept, -imag), (-turned_m, real_m), (kept_m, imag_m),
    )
    for n, (first, second) in enumerate(factors):
        mixed_ref[s, n] = jnp.where(even, first, second)


def power_rows(rows):
    power = jnp.sum(jnp.sum(rows * rows, axis=0, keepdims=True), axis=1, keepdims=True)
    high = power.astype(jnp.bfloat16).astype(jnp.float32)
    return jnp.concatenate([jnp.broadcast_to(x, (1, LANES)) for x in (high, power - high)], 0)


def tables_kernel(
    tm_count, bands_half, width, seg_kept,
    valid_hbm, table_hbm, lags_hbm, drift_hbm,
    inner_ref, outer_ref, picks_ref,
    valid_ref, table_ref, lags_ref, drift_ref, sems,
):
    bin_half, detector_bit = duty()
    copies = fetch((valid_hbm, table_hbm, lags_hbm, drift_hbm), (valid_ref, table_ref, lags_ref, drift_ref), sems)
    inner_at, start_at = inner_rows(), start_rows(width // INNER)
    for copy in copies:
        copy.wait()
    marks = clock(valid_ref, tm_count, detector_bit, seg_kept)

    def one_slot(slot):
        row = block_of(slot, table_ref, tm_count, bin_half)
        band = table_ref[0, row]
        frequency = (band * width).astype(jnp.float32) + start_at
        share = (band.astype(jnp.float32) + 0.5) / (2 * bands_half)
        picks_ref[slot : slot + 1, :] = jnp.full((1, LANES), band - bin_half * bands_half)
        for m in range(TPB):
            tile = table_ref[1, row + m]
            at = slot * TPB + m
            picks_ref[slots + at : slots + at + 1, :] = jnp.full((1, LANES), tile)
            lag, parts = inner_tables(tile, lags_ref, inner_at)
            inner_ref[at] = parts
            for s, (live, time) in enumerate(marks):
                cosine, sine = outer_tables(tile, lag, drift_ref, share * time, frequency, live)
                outer_ref[at, s, 0] = cosine
                outer_ref[at, s, 1] = sine

    slots = inner_ref.shape[0] // TPB
    over_slots(slots, one_slot)


def mix_kernel(seg_kept, picks_ref, own_ref, mixed_ref, power_ref, rows32, masked):
    _, detector_bit = duty()
    _, outer = mixed_ref.shape[2:4]
    flip = jnp.where(detector_bit == 0, 1.0, -1.0).astype(jnp.float32)

    def band_of(slot):
        return picks_ref[slot : slot + 1, :][0, 0]

    for s in range(seg_kept):
        rows32[...] = own_ref[detector_bit * seg_kept + s].astype(jnp.float32)
        power_ref[s] = power_rows(rows32[...])
        mix_own(rows32, band_of, masked, mixed_ref, s, flip, outer, own_ref.shape[2])


def terms_kernel(tm_count, dests, rows_dest, seg_kept, ready, *refs):
    if ready:
        inner_ref, outer_ref, picks_ref, mixed_ref, power_ref, other_ref, out_ref, *scratch = refs
        copies = ()
    else:
        valid_hbm, table_hbm, lags_hbm, drift_hbm, own_ref, other_ref, out_ref, *scratch = refs
        valid_ref, table_ref, lags_ref, drift_ref, sems, mixed_ref, *scratch = scratch
        copies = fetch((valid_hbm, table_hbm, lags_hbm, drift_hbm), (valid_ref, table_ref, lags_ref, drift_ref), sems)
    rows32, masked, left, total = scratch
    bin_half, detector_bit = duty()
    bands_half = other_ref.shape[1] // 2
    width = other_ref.shape[2]
    outer = width // INNER
    per_tile = PT // LANES
    slots = masked.shape[0]
    flip = jnp.where(detector_bit == 0, 1.0, -1.0).astype(jnp.float32)
    part = lax.broadcasted_iota(jnp.int32, (slots, outer, LANES), 2) // HALF
    total[...] = jnp.zeros_like(total)

    def band_of(slot):
        if ready:
            return picks_ref[slot : slot + 1, :][0, 0]
        return table_ref[0, block_of(slot, table_ref, tm_count, bin_half)] - bin_half * bands_half

    def tile_of(at):
        if ready:
            return picks_ref[slots + at : slots + at + 1, :][0, 0]
        return table_ref[1, block_of(at // TPB, table_ref, tm_count, bin_half) + at % TPB]

    for s in range(seg_kept):
        seg = detector_bit * seg_kept + s
        rows32[...] = other_ref[seg].astype(jnp.float32)
        powers = [power_ref[s] if ready else power_rows(own_ref[seg].astype(jnp.float32)), power_rows(rows32[...])]
        if s == 0:
            for copy in copies:
                copy.wait()
        wide = spread(rows32, band_of, masked, outer, width, gather=ready)
        if not ready:
            rows32[...] = own_ref[seg].astype(jnp.float32)
            mix_own(rows32, band_of, masked, mixed_ref, s, flip, outer, width)
            inner_at, start_at = inner_rows(), start_rows(outer)
            live, time = clock(valid_ref, tm_count, detector_bit, seg_kept)[s]
        sides = []
        for n in range(2):
            value = sum(mixed_ref[s, 4 * n + q] * wide[q] for q in range(4))
            high = value.astype(jnp.bfloat16).astype(jnp.float32)
            sides.append(jnp.where((part == 2) | (part == 3), value - high, high))
        lefts = jnp.concatenate(sides, 1).astype(jnp.bfloat16)
        if not ready:
            left[...] = lefts

        def one_slot(slot):
            lhs = (lefts if ready else left)[slot][:, : PARTS * HALF]
            for m in range(TPB):
                at = slot * TPB + m
                tile = tile_of(at)
                if ready:
                    table = inner_ref[at]
                    cosine, sine = outer_ref[at, s, 0], outer_ref[at, s, 1]
                else:
                    band = band_of(slot) + bin_half * bands_half
                    lag, table = inner_tables(tile, lags_ref, inner_at)
                    turn = (band.astype(jnp.float32) + 0.5) / (2 * bands_half) * time
                    frequency = (band * width).astype(jnp.float32) + start_at
                    cosine, sine = outer_tables(tile, lag, drift_ref, turn, frequency, live)
                rhs = jnp.concatenate([table[:INNER], table], 0)
                product = jnp.dot(lhs, rhs, preferred_element_type=jnp.float32)
                terms = jnp.sum(cosine * product[:outer] - sine * product[outer:], axis=0, keepdims=True)
                total[s, tile] += jnp.concatenate([terms[:, c * LANES : (c + 1) * LANES] for c in range(per_tile)], 0)

        over_slots(slots, one_slot)
        tiles = rows_dest // per_tile
        powers = jnp.concatenate(powers, 0)
        for d in range(dests):
            piece = total[s, d * tiles : (d + 1) * tiles].reshape(rows_dest, LANES)
            out_ref[d, s] = jnp.concatenate([piece, powers], 0).astype(jnp.bfloat16)


def weights_of(power, fourier_bins):
    halves = power[..., 0::2, :] + power[..., 1::2, :]
    whole = halves.reshape(2, 2, *halves.shape[1:]).sum(1) / fourier_bins + 1e-06
    return 1.0 / (whole[..., 0, :] * whole[..., 1, :])


def sum_kernel(tm_count, rows_dest, fourier_bins, scale, got_ref, out_ref):
    seg_kept = got_ref.shape[1]
    total = jnp.zeros((rows_dest, LANES), jnp.float32)
    for k in range(2):
        for i in range(tm_count):
            for s in range(seg_kept):
                pair = [got_ref[(2 * k + h) * tm_count + i, s].astype(jnp.float32) for h in range(2)]
                both = pair[0] + pair[1]
                own = (both[rows_dest : rows_dest + 1] + both[rows_dest + 1 : rows_dest + 2]) / fourier_bins + 1e-06
                other = (both[rows_dest + 2 : rows_dest + 3] + both[rows_dest + 3 : rows_dest + 4]) / fourier_bins + 1e-06
                total = total + both[:rows_dest] * (1.0 / (own * other))
    out_ref[...] = total / scale


def shards(spectra, valid, lags, drift, block_table):
    det_count, tm_count = lax.axis_size("det"), lax.axis_size("tm")
    devices = det_count * tm_count
    own = spectra[0]
    seg_count, bands_half, _, width = own.shape
    seg_kept = seg_count // 2
    pixels = lags.shape[0]
    per_device = pixels // devices
    fourier_bins = 2 * bands_half * width
    scale = math.sqrt(seg_count * tm_count * width)
    direct = per_device % PT == 0
    rows_dest = (per_device if direct else pixels) // LANES
    dests = devices if direct else 1
    rows = rows_dest + 4
    per_tile = PT // LANES
    blocks = block_table.shape[0] // 2
    slots = blocks // TPB
    outer = width // INNER

    own = own.reshape(seg_count, 2 * bands_half, width)
    other = lax.ppermute(own, "det", [(d, d ^ 3) for d in range(det_count)])
    own = lax.ppermute(own, "det", [(d, d ^ 1) for d in range(det_count)])
    table = block_table.T
    lags, drift = (x.reshape(-1, per_tile, LANES) for x in (lags, drift))
    settings = tuple(pltpu.with_memory_space_constraint(x, pltpu.HBM) for x in (valid, table, lags, drift))
    held = [pltpu.SMEM(valid.shape, jnp.int32), pltpu.SMEM(table.shape, jnp.int32)]
    held += [pltpu.VMEM(lags.shape, jnp.float32), pltpu.VMEM(drift.shape, jnp.float32)]
    work = [pltpu.VMEM(own.shape[1:], jnp.float32), pltpu.VMEM((slots, 2 * outer, width), jnp.bfloat16)]
    mixed = jax.ShapeDtypeStruct((seg_kept, 8, slots, outer, LANES), jnp.float32)
    ready = slots <= UNROLLED
    if ready:
        made = pl.pallas_call(
            functools.partial(tables_kernel, tm_count, bands_half, width, seg_kept),
            out_shape=[
                jax.ShapeDtypeStruct((blocks, 2 * INNER, PT), jnp.bfloat16),
                jax.ShapeDtypeStruct((blocks, seg_kept, 2, outer, PT), jnp.float32),
                jax.ShapeDtypeStruct((slots + blocks, LANES), jnp.int32),
            ],
            in_specs=[HBM] * 4,
            out_specs=[VMEM] * 3,
            scratch_shapes=[*held, pltpu.SemaphoreType.DMA((4,))],
            compiler_params=GRANT,
            cost_estimate=pl.CostEstimate(flops=10**9, bytes_accessed=10**6, transcendentals=0),
            name="tables",
        )(*settings)
        factors = pl.pallas_call(
            functools.partial(mix_kernel, seg_kept),
            out_shape=[mixed, jax.ShapeDtypeStruct((seg_kept, 2, LANES), jnp.float32)],
            in_specs=[VMEM] * 2,
            out_specs=[VMEM] * 2,
            scratch_shapes=work,
            compiler_params=GRANT,
            cost_estimate=pl.CostEstimate(flops=10**8, bytes_accessed=10**6, transcendentals=0),
            name="mix",
        )(made[2], own)
        settings, held = (*made, *factors), []
    else:
        settings = (*settings, own)
        held += [pltpu.SemaphoreType.DMA((4,)), pltpu.VMEM(mixed.shape, mixed.dtype)]
    outgoing = pl.pallas_call(
        functools.partial(terms_kernel, tm_count, dests, rows_dest, seg_kept, ready),
        out_shape=jax.ShapeDtypeStruct((dests, seg_kept, rows, LANES), jnp.bfloat16),
        in_specs=([VMEM] * 5 if ready else [HBM] * 4 + [VMEM]) + [VMEM],
        out_specs=VMEM,
        scratch_shapes=[
            *held,
            *work,
            pltpu.VMEM((slots, 2 * outer, LANES), jnp.bfloat16),
            pltpu.VMEM((seg_kept, pixels // PT, per_tile, LANES), jnp.float32),
        ],
        compiler_params=GRANT if ready else None,
        name="terms",
    )(*settings, other)
    if direct:
        received = lax.all_to_all(outgoing, ("det", "tm"), 0, 0, tiled=True)
        result = pl.pallas_call(
            functools.partial(sum_kernel, tm_count, rows_dest, fourier_bins, scale),
            out_shape=jax.ShapeDtypeStruct((rows_dest, LANES), jnp.float32),
            in_specs=[VMEM],
            out_specs=VMEM,
            compiler_params=GRANT,
            name="sum",
        )(received)
        return result.reshape(-1)
    maps = jnp.moveaxis(outgoing[0, :, :rows_dest].reshape(seg_kept, devices, per_device), 1, 0)
    powers = jnp.broadcast_to(outgoing[0, :, rows_dest : rows_dest + 4, 0], (devices, seg_kept, 4))
    sent = jnp.concatenate([maps, powers], 2)
    received = lax.all_to_all(sent, ("det", "tm"), 0, 0, tiled=True).astype(jnp.float32)
    received = received.reshape(det_count, tm_count, seg_kept, per_device + 4)
    weight = weights_of(received[..., per_device:, None], fourier_bins)[..., 0]
    both = received[..., :per_device].reshape(2, 2, tm_count, seg_kept, per_device).sum(1)
    return (both * weight[..., None]).sum((0, 1, 2)) / scale


def solution(mesh):
    placed = (P("det", "tm", None, None, None), P("tm"), P(), P(), P())
    return jax.shard_map(
        shards, mesh=mesh, in_specs=placed, out_specs=P(("det", "tm")), check_vma=False
    )
```
